128 devices in a mesh: graph: 128 (over z, y, x, core).
Axes of the slice: x: 4, y: 4, z: 4, core: 2. Of those that a mesh axis runs over, the one named last changes fastest.
Arguments:
- feats: bfloat16 [524288, 768], P('graph')
- w_one: float32 [768, 1024], replicated
- w_two: float32 [1024, 153], replicated
- send_idx: int32 [16384, 4], P('graph')
- send_count: int32 [16384], P('graph')
- edge_src: int32 [524288, 8], P('graph')
- edge_wt: float32 [524288, 8], P('graph')
- labels: int32 [524288], P('graph')
- label_mask: int32 [524288], P('graph')
Outputs:
- output 1: float32 [], replicated
- output 2: float32 [768, 1024], replicated
- output 3: float32 [1024, 153], replicated
All inputs are finite; a program needn't handle non-finite values.
Results may differ from the reference program's by a relative error of at most 0.001.
Values are sent between devices in bfloat16 or wider.
A program may use at most 1 GiB of HBM per device.

```python
import jax
import jax.numpy as jnp
from jax import lax

GRAPH_DEVS = 128
ROWS_DEV = 4096
HALO_ROWS = 4
IN_DEG = 8
FEAT_IN = 768
FEAT_HID = 1024
CLASSES = 153

TOTAL_ROWS = GRAPH_DEVS * ROWS_DEV
EXT_ROWS = ROWS_DEV + GRAPH_DEVS * HALO_ROWS


def draw_structure(rng_key):
    rng_keys = jax.random.split(rng_key, 7)
    dev_ids = jnp.arange(GRAPH_DEVS)
    skew_a = jax.random.randint(rng_keys[0], (GRAPH_DEVS, GRAPH_DEVS), 0, HALO_ROWS)
    skew_b = jax.random.randint(rng_keys[1], (GRAPH_DEVS, GRAPH_DEVS), 0, HALO_ROWS)
    counts = 1 + (skew_a * skew_b) // HALO_ROWS
    full_list = dev_ids[None, :] == (dev_ids[:, None] + 1) % GRAPH_DEVS
    counts = jnp.where(full_list, HALO_ROWS, counts)
    send_idx = jax.random.randint(rng_keys[2], (GRAPH_DEVS * GRAPH_DEVS, HALO_ROWS), 0, ROWS_DEV)
    edge_shape = (GRAPH_DEVS, ROWS_DEV, IN_DEG)
    is_cut = jax.random.randint(rng_keys[3], edge_shape, 0, 4) == 0
    local_src = jax.random.randint(rng_keys[4], edge_shape, 0, ROWS_DEV)
    peer_dev = (dev_ids[:, None, None] + jax.random.randint(rng_keys[5], edge_shape, 1, GRAPH_DEVS)) % GRAPH_DEVS
    peer_count = counts[peer_dev, dev_ids[:, None, None]]
    slot_pos = jax.random.randint(rng_keys[6], edge_shape, 0, 1048576) % peer_count
    halo_src = ROWS_DEV + peer_dev * HALO_ROWS + slot_pos
    edge_src = jnp.where(is_cut, halo_src, local_src).reshape(TOTAL_ROWS, IN_DEG)
    return send_idx, counts.reshape(GRAPH_DEVS * GRAPH_DEVS), edge_src, is_cut.reshape(TOTAL_ROWS, IN_DEG)


def setup_inputs(seed: int = 0) -> dict:
    rng_keys = jax.random.split(jax.random.key(seed), 7)
    feats = jax.random.normal(rng_keys[0], (TOTAL_ROWS, FEAT_IN), jnp.float32).astype(jnp.bfloat16)
    w_one = jax.random.normal(rng_keys[1], (FEAT_IN, FEAT_HID), jnp.float32) * FEAT_IN ** -0.5
    w_two = jax.random.normal(rng_keys[2], (FEAT_HID, CLASSES), jnp.float32) * FEAT_HID ** -0.5
    send_idx, send_count, edge_src, is_cut = draw_structure(rng_keys[3])
    raw_wt = jax.random.uniform(rng_keys[4], (TOTAL_ROWS, IN_DEG), jnp.float32, 0.5, 1.5) * jnp.where(is_cut, 0.5, 1.0)
    edge_wt = raw_wt / jnp.sqrt(jnp.sum(raw_wt * raw_wt, axis=1, keepdims=True))
    labels = jax.random.randint(rng_keys[5], (TOTAL_ROWS,), 0, CLASSES)
    label_mask = jax.random.randint(rng_keys[6], (TOTAL_ROWS,), 0, 2)
    return {"feats": feats, "w_one": w_one, "w_two": w_two, "send_idx": send_idx, "send_count": send_count, "edge_src": edge_src, "edge_wt": edge_wt, "labels": labels, "label_mask": label_mask}


def reference(feats, w_one, w_two, send_idx, send_count, edge_src, edge_wt, labels, label_mask):
    dev_ids = jnp.arange(GRAPH_DEVS)
    send_lists = send_idx.reshape(GRAPH_DEVS, GRAPH_DEVS, HALO_ROWS) + (dev_ids * ROWS_DEV)[:, None, None]
    is_valid = (jnp.arange(HALO_ROWS)[None, None, :] < send_count.reshape(GRAPH_DEVS, GRAPH_DEVS)[:, :, None]).astype(jnp.float32)
    halo_ids = jnp.transpose(send_lists, (1, 0, 2)).reshape(GRAPH_DEVS, GRAPH_DEVS * HALO_ROWS)
    halo_ok = jnp.transpose(is_valid, (1, 0, 2)).reshape(GRAPH_DEVS, GRAPH_DEVS * HALO_ROWS)
    src_dev = edge_src.reshape(GRAPH_DEVS, ROWS_DEV, IN_DEG)
    wt_dev = edge_wt.reshape(GRAPH_DEVS, ROWS_DEV, IN_DEG)

    def aggregate(h_flat):
        feat_width = h_flat.shape[1]

        def one_dev(per_dev):
            own_rows, src_ids, edge_w, ids_here, ok_here = per_dev
            halo_vals = h_flat[ids_here].astype(jnp.float32) * ok_here[:, None]
            ext_rows = jnp.concatenate([own_rows.astype(jnp.float32), halo_vals], axis=0)
            return jnp.sum(ext_rows[src_ids] * edge_w[:, :, None], axis=1)

        blocks = h_flat.reshape(GRAPH_DEVS, ROWS_DEV, feat_width)
        return lax.map(one_dev, (blocks, src_dev, wt_dev, halo_ids, halo_ok)).reshape(TOTAL_ROWS, feat_width)

    def scatter_back(d_z):
        feat_width = d_z.shape[1]

        def one_dev(per_dev):
            src_ids, edge_w, dz_rows = per_dev
            contrib = (edge_w[:, :, None] * dz_rows[:, None, :]).reshape(ROWS_DEV * IN_DEG, feat_width)
            return jax.ops.segment_sum(contrib, src_ids.reshape(ROWS_DEV * IN_DEG), num_segments=EXT_ROWS)

        ext_grad = lax.map(one_dev, (src_dev, wt_dev, d_z.reshape(GRAPH_DEVS, ROWS_DEV, feat_width)))
        own_grad = ext_grad[:, :ROWS_DEV].reshape(TOTAL_ROWS, feat_width)
        halo_grad = ext_grad[:, ROWS_DEV:] * halo_ok[:, :, None]
        back_sum = jax.ops.segment_sum(halo_grad.reshape(GRAPH_DEVS * GRAPH_DEVS * HALO_ROWS, feat_width), halo_ids.reshape(GRAPH_DEVS * GRAPH_DEVS * HALO_ROWS), num_segments=TOTAL_ROWS)
        return own_grad + back_sum

    w_one_b = w_one.astype(jnp.bfloat16)
    w_two_b = w_two.astype(jnp.bfloat16)
    z_one = aggregate(feats).astype(jnp.bfloat16)
    h_one = jnp.maximum(jnp.dot(z_one, w_one_b, preferred_element_type=jnp.float32), 0.0).astype(jnp.bfloat16)
    z_two = aggregate(h_one).astype(jnp.bfloat16)
    logits = jnp.dot(z_two, w_two_b, preferred_element_type=jnp.float32)
    mask_f = label_mask.astype(jnp.float32)
    label_total = jnp.sum(mask_f)
    log_prob = jax.nn.log_softmax(logits, axis=-1)
    onehot = (labels[:, None] == jnp.arange(CLASSES)[None, :]).astype(jnp.float32)
    loss_val = -jnp.sum(mask_f[:, None] * onehot * log_prob) / label_total
    d_logits = ((jnp.exp(log_prob) - onehot) * (mask_f / label_total)[:, None]).astype(jnp.bfloat16)
    grad_two = jnp.dot(z_two.T, d_logits, preferred_element_type=jnp.float32)
    d_z2 = jnp.dot(d_logits, w_two_b.T, preferred_element_type=jnp.float32)
    d_h1 = scatter_back(d_z2)
    d_y1 = jnp.where(h_one > 0, d_h1, 0.0).astype(jnp.bfloat16)
    grad_one = jnp.dot(z_one.T, d_y1, preferred_element_type=jnp.float32)
    return (loss_val, grad_one, grad_two)
```

```python
import functools

import jax
import jax.numpy as jnp
from jax import lax
from jax.experimental import pallas as pl
from jax.experimental.pallas import tpu as pltpu
from jax.sharding import PartitionSpec as P

LANES = 128
STEP = 16
BLOCK = 256
F32, BF16 = jnp.float32, jnp.bfloat16


def once(shape):
    return pl.BlockSpec(shape, lambda g: (0,) * len(shape), pipeline_mode=pl.Buffered(1))


def fill_rows(dst, src, offset, blocks):
    def step(i, carry):
        r = pl.multiple_of(i * 64, 64)
        x = src[pl.ds(r, 64), :].astype(F32)
        for c in range(blocks):
            dst[pl.ds((r + offset) * 8 + c, 64, stride=8), :] = x[:, c * LANES : (c + 1) * LANES]
        return carry

    lax.fori_loop(0, src.shape[0] // 64, step, 0)


def spread_weights(w, deg):
    return tuple(jnp.broadcast_to(w[h * 8 : h * 8 + 8, k : k + 1], (8, LANES)) for h in range(STEP // 8) for k in range(deg))


def gather_rows(first_step, steps, src, wt, table, out, wbuf):
    deg = wt.shape[1]

    def weights_at(i):
        return spread_weights(wt[pl.ds(pl.multiple_of(i * STEP, STEP), STEP), :], deg)

    def step(i, tiles):
        for t, tile in enumerate(tiles):
            wbuf[pl.ds(t * 8, 8), :] = tile
        ahead = weights_at(jnp.minimum(i + 1, steps - 1))
        dst = out.at[pl.ds(pl.multiple_of(i * STEP * 8, STEP * 8), STEP * 8)]
        for u in range(STEP):
            acc = None
            for k in range(deg):
                row = table[pl.ds(pl.multiple_of(src[u * deg + k, first_step + i], 8), 8), :]
                term = row * wbuf[pl.ds((u // 8 * deg + k) * 8 + u % 8, 8, stride=0), :]
                acc = term if acc is None else acc + term
            dst[pl.ds(u * 8, 8), :] = acc
        return ahead

    lax.fori_loop(0, steps, step, weights_at(0))


def layer_one_kernel(src, wt, own, halo, w, z_out, h_out, table, zbuf, wbuf):
    g = pl.program_id(0)
    rows, blocks = z_out.shape[0], own.shape[1] // LANES

    @pl.when(g == 0)
    def _():
        fill_rows(table, own, 0, blocks)
        fill_rows(table, halo, own.shape[0], blocks)

    steps = rows // STEP
    gather_rows(g * steps, steps, src, wt, table, zbuf, wbuf)
    z = jnp.concatenate([zbuf[pl.ds(c, rows, stride=8), :] for c in range(blocks)], axis=1).astype(BF16)
    z_out[...] = z
    y = jnp.dot(z, w[...], preferred_element_type=F32)
    h_out[...] = jnp.maximum(y, 0.0).astype(BF16)


def layer_two_kernel(classes, src, inv_total, wt, own, halo, w, label, g_out, gw_out, loss_out, table, zbuf, wbuf):
    g = pl.program_id(0)
    rows, blocks = g_out.shape[0], own.shape[1] // LANES

    @pl.when(g == 0)
    def _():
        fill_rows(table, own, 0, blocks)
        fill_rows(table, halo, own.shape[0], blocks)
        gw_out[...] = jnp.zeros_like(gw_out)
        loss_out[...] = jnp.zeros_like(loss_out)

    steps = rows // STEP
    gather_rows(g * steps, steps, src, wt, table, zbuf, wbuf)
    z = jnp.concatenate([zbuf[pl.ds(c, rows, stride=8), :] for c in range(blocks)], axis=1).astype(BF16)
    logits = jnp.dot(z, w[...], preferred_element_type=F32)
    col = lax.broadcasted_iota(jnp.int32, logits.shape, 1)
    real = col < classes
    top = jnp.max(jnp.where(real, logits, -jnp.inf), axis=1, keepdims=True)
    shifted = logits - top
    log_sum = jnp.log(jnp.sum(jnp.where(real, jnp.exp(shifted), 0.0), axis=1, keepdims=True))
    log_prob = shifted - log_sum
    tag = label[...]
    hit = col == tag
    loss_out[...] += jnp.sum(jnp.where(hit, log_prob, 0.0), axis=(0, 1), keepdims=True)
    scale = jnp.where(tag >= 0, inv_total[0], 0.0)
    grad = jnp.where(real, (jnp.exp(log_prob) - jnp.where(hit, 1.0, 0.0)) * scale, 0.0).astype(BF16)
    g_out[...] = grad
    gw_out[...] += lax.dot_general(grad, z, (((0,), (0,)), ((), ())), preferred_element_type=F32)


def scatter_kernel(src, wt, grad, s_out, gbuf, wbuf, *parts):
    g = pl.program_id(0)
    rows, deg = grad.shape[0], wt.shape[1]
    steps = rows // STEP

    @pl.when(g == 0)
    def _():
        def clear(i, carry):
            for part in parts:
                for j in range(8):
                    part[pl.ds(pl.multiple_of(i * 64, 64) + j * 8, 8), :] = jnp.zeros((8, LANES), F32)
            return carry

        lax.fori_loop(0, s_out.shape[0] // 64, clear, 0)

    x = grad[...].astype(F32)
    for c in range(2):
        gbuf[pl.ds(c, rows, stride=2), :] = x[:, c * LANES : (c + 1) * LANES]

    def weights_at(i):
        return spread_weights(wt[pl.ds(pl.multiple_of(i * STEP, STEP), STEP), :], deg)

    def step(i, tiles):
        for t, tile in enumerate(tiles):
            wbuf[pl.ds(t * 8, 8), :] = tile
        ahead = weights_at(jnp.minimum(i + 1, steps - 1))
        here = gbuf.at[pl.ds(pl.multiple_of(i * STEP * 2, STEP * 2), STEP * 2)]
        for u in range(STEP):
            row = here[pl.ds(u * 2, 2), :]
            for k in range(deg):
                at = pl.ds(pl.multiple_of(src[u * deg + k, g * steps + i], 2), 2)
                w = wbuf[pl.ds((u // 8 * deg + k) * 8 + u % 8, 2, stride=0), :]
                parts[k][at, :] = parts[k][at, :] + row * w
        return ahead

    lax.fori_loop(0, steps, step, weights_at(0))

    @pl.when(g == pl.num_programs(0) - 1)
    def _():
        def add(i, carry):
            at = pl.ds(pl.multiple_of(i * 64, 64), 64)
            total = parts[0][at, :]
            for part in parts[1:]:
                total = total + part[at, :]
            s_out[at, :] = total
            return carry

        lax.fori_loop(0, s_out.shape[0] // 64, add, 0)


def backward_kernel(lists, own, back, w_t, h, z, gw_out, total):
    g = pl.program_id(0)
    rows = h.shape[0]

    @pl.when(g == 0)
    def _():
        gw_out[...] = jnp.zeros_like(gw_out)

        def copy(i, carry):
            at = pl.ds(pl.multiple_of(i * 64, 64), 64)
            total[at, :] = own[at, :]
            return carry

        lax.fori_loop(0, own.shape[0] // 64, copy, 0)

        def add(i, carry):
            for j in range(4):
                at = pl.ds(pl.multiple_of(lists[i * 4 + j], 2), 2)
                total[at, :] = total[at, :] + back[pl.ds(pl.multiple_of(i * 8, 8) + j * 2, 2), :]
            return carry

        lax.fori_loop(0, back.shape[0] // 8, add, 0)

    s = jnp.concatenate([total[pl.ds(g * rows * 2 + c, rows, stride=2), :] for c in range(2)], axis=1)
    high = s.astype(BF16)
    rest = s - high.astype(F32)
    mid = rest.astype(BF16)
    low = (rest - mid.astype(F32)).astype(BF16)
    wt = w_t[...]
    d = jnp.dot(low, wt, preferred_element_type=F32)
    d = d + jnp.dot(mid, wt, preferred_element_type=F32)
    d = d + jnp.dot(high, wt, preferred_element_type=F32)
    grad = jnp.where(h[...] > 0, d, 0.0).astype(BF16)
    gw_out[...] += lax.dot_general(z[...], grad, (((0,), (0,)), ((), ())), preferred_element_type=F32)


def params():
    return pltpu.CompilerParams(dimension_semantics=("arbitrary",), vmem_limit_bytes=62 * 2**20)


SMEM = pl.BlockSpec(memory_space=pltpu.SMEM)


def solution(mesh):
    dev_count = mesh.shape["graph"]

    def device_step(feats, w_one, w_two, send_idx, send_count, edge_src, edge_wt, labels, label_mask):
        n, f_in = feats.shape
        f_hid, classes = w_two.shape
        halo_rows, deg = send_idx.shape[1], edge_src.shape[1]
        halo = dev_count * halo_rows
        ext = n + halo
        pad = 2 * LANES
        w_one_b = w_one.astype(BF16)
        w_two_b = jnp.pad(w_two.astype(BF16), ((0, 0), (0, pad - classes)))
        list_ids = send_idx.reshape(halo)
        list_ok = jnp.arange(halo_rows)[None, :] < send_count[:, None]
        src_t = edge_src.reshape(n // STEP, STEP * deg).T
        src8, src2 = src_t * 8, src_t * 2
        lists2 = jnp.where(list_ok, send_idx, n).reshape(halo) * 2
        label = jnp.where(label_mask == 1, labels, -1).reshape(n, 1)
        label_total = lax.psum(jnp.sum(label_mask.astype(F32)), "graph")
        inv_total = (1.0 / label_total).reshape(1)
        ok_rows = list_ok.reshape(halo, 1)

        def exchange(h_rows):
            outgoing = jnp.where(ok_rows, h_rows[list_ids], 0)
            return lax.all_to_all(outgoing, "graph", 0, 0, tiled=True)

        def by_rows(width):
            return pl.BlockSpec((BLOCK, width), lambda g: (g, 0))

        gather_scratch = [
            pltpu.VMEM((ext * 8, LANES), F32),
            pltpu.VMEM((BLOCK * 8, LANES), F32),
            pltpu.VMEM((STEP * deg + 8, LANES), F32),
        ]
        z_one, h_one = pl.pallas_call(
            layer_one_kernel,
            grid=(n // BLOCK,),
            in_specs=[SMEM, by_rows(deg), once((n, f_in)), once((halo, f_in)), once((f_in, f_hid))],
            out_specs=[by_rows(f_in), by_rows(f_hid)],
            out_shape=[jax.ShapeDtypeStruct((n, f_in), BF16), jax.ShapeDtypeStruct((n, f_hid), BF16)],
            scratch_shapes=gather_scratch,
            compiler_params=params(),
            name="layer_one",
        )(src8, edge_wt, feats, exchange(feats), w_one_b)
        grad_log, gw_two, loss_sum = pl.pallas_call(
            functools.partial(layer_two_kernel, classes),
            grid=(n // BLOCK,),
            in_specs=[SMEM, SMEM, by_rows(deg), once((n, f_hid)), once((halo, f_hid)), once((f_hid, pad)), by_rows(1)],
            out_specs=[by_rows(pad), once((pad, f_hid)), once((1, 1))],
            out_shape=[
                jax.ShapeDtypeStruct((n, pad), BF16),
                jax.ShapeDtypeStruct((pad, f_hid), F32),
                jax.ShapeDtypeStruct((1, 1), F32),
            ],
            scratch_shapes=gather_scratch,
            compiler_params=params(),
            name="layer_two",
        )(src8, inv_total, edge_wt, h_one, exchange(h_one), w_two_b, label)
        ext_grad = pl.pallas_call(
            scatter_kernel,
            grid=(n // 512,),
            in_specs=[SMEM, pl.BlockSpec((512, deg), lambda g: (g, 0)), pl.BlockSpec((512, pad), lambda g: (g, 0))],
            out_specs=once((ext * 2, LANES)),
            out_shape=jax.ShapeDtypeStruct((ext * 2, LANES), F32),
            scratch_shapes=[pltpu.VMEM((512 * 2, LANES), F32), pltpu.VMEM((STEP * deg + 8, LANES), F32)]
            + [pltpu.VMEM((ext * 2, LANES), F32) for _ in range(deg)],
            compiler_params=params(),
            name="scatter",
        )(src2, edge_wt, grad_log)
        back = lax.all_to_all(ext_grad[n * 2 :], "graph", 0, 0, tiled=True)
        gw_one = pl.pallas_call(
            backward_kernel,
            grid=(n // 512,),
            in_specs=[
                SMEM,
                once((n * 2, LANES)),
                once((halo * 2, LANES)),
                once((pad, f_hid)),
                pl.BlockSpec((512, f_hid), lambda g: (g, 0)),
                pl.BlockSpec((512, f_in), lambda g: (g, 0)),
            ],
            out_specs=once((f_in, f_hid)),
            out_shape=jax.ShapeDtypeStruct((f_in, f_hid), F32),
            scratch_shapes=[pltpu.VMEM((n * 2 + 8, LANES), F32)],
            compiler_params=params(),
            name="backward",
        )(lists2, ext_grad, back, w_two_b.T, h_one, z_one)
        loss_sum, gw_one, gw_two = lax.psum((loss_sum[0, 0], gw_one, gw_two[:classes].T), "graph")
        return -loss_sum / label_total, gw_one, gw_two

    row_spec = P("graph", None)
    vec_spec = P("graph")
    return jax.shard_map(
        device_step,
        mesh=mesh,
        in_specs=(row_spec, P(), P(), row_spec, vec_spec, row_spec, row_spec, vec_spec, vec_spec),
        out_specs=(P(), P(), P()),
        check_vma=False,
    )
```

```python
import functools

import jax
import jax.numpy as jnp
from jax import lax
from jax.experimental import pallas as pl
from jax.experimental.pallas import tpu as pltpu
from jax.sharding import PartitionSpec as P

LANES = 128
STEP = 16
BLOCK = 256
F32, BF16 = jnp.float32, jnp.bfloat16


def once(shape):
    return pl.BlockSpec(shape, lambda g: (0,) * len(shape), pipeline_mode=pl.Buffered(1))


def fill_rows(dst, src, offset, blocks):
    def step(i, carry):
        r = pl.multiple_of(i * 64, 64)
        x = src[pl.ds(r, 64), :].astype(F32)
        for c in range(blocks):
            dst[pl.ds((r + offset) * 8 + c, 64, stride=8), :] = x[:, c * LANES : (c + 1) * LANES]
        return carry

    lax.fori_loop(0, src.shape[0] // 64, step, 0)


def spread_weights(w, deg):
    return tuple(jnp.broadcast_to(w[h * 8 : h * 8 + 8, k : k + 1], (8, LANES)) for h in range(STEP // 8) for k in range(deg))


def gather_rows(first_step, steps, src, wt, table, out, wbuf):
    deg = wt.shape[1]

    def weights_at(i):
        return spread_weights(wt[pl.ds(pl.multiple_of(i * STEP, STEP), STEP), :], deg)

    def step(i, tiles):
        for t, tile in enumerate(tiles):
            wbuf[pl.ds(t * 8, 8), :] = tile
        ahead = weights_at(jnp.minimum(i + 1, steps - 1))
        dst = out.at[pl.ds(pl.multiple_of(i * STEP * 8, STEP * 8), STEP * 8)]
        for u in range(STEP):
            acc = None
            for k in range(deg):
                row = table[pl.ds(pl.multiple_of(src[u * deg + k, first_step + i], 8), 8), :]
                term = row * wbuf[pl.ds((u // 8 * deg + k) * 8 + u % 8, 8, stride=0), :]
                acc = term if acc is None else acc + term
            dst[pl.ds(u * 8, 8), :] = acc
        return ahead

    lax.fori_loop(0, steps, step, weights_at(0))


def layer_one_kernel(src, wt, own, halo, w, z_out, h_out, table, zbuf, wbuf):
    g = pl.program_id(0)
    rows, blocks = z_out.shape[0], own.shape[1] // LANES

    @pl.when(g == 0)
    def _():
        fill_rows(table, own, 0, blocks)
        fill_rows(table, halo, own.shape[0], blocks)

    steps = rows // STEP
    gather_rows(g * steps, steps, src, wt, table, zbuf, wbuf)
    z = jnp.concatenate([zbuf[pl.ds(c, rows, stride=8), :] for c in range(blocks)], axis=1).astype(BF16)
    z_out[...] = z
    y = jnp.dot(z, w[...], preferred_element_type=F32)
    h_out[...] = jnp.maximum(y, 0.0).astype(BF16)


def layer_two_kernel(classes, src, inv_total, wt, own, halo, w, label, g_out, gw_out, table, zbuf, wbuf, loss_sum):
    g = pl.program_id(0)
    rows, blocks = g_out.shape[0], own.shape[1] // LANES

    @pl.when(g == 0)
    def _():
        fill_rows(table, own, 0, blocks)
        fill_rows(table, halo, own.shape[0], blocks)
        gw_out[...] = jnp.zeros_like(gw_out)
        loss_sum[...] = jnp.zeros_like(loss_sum)

    steps = rows // STEP
    gather_rows(g * steps, steps, src, wt, table, zbuf, wbuf)
    z = jnp.concatenate([zbuf[pl.ds(c, rows, stride=8), :] for c in range(blocks)], axis=1).astype(BF16)
    logits = jnp.dot(z, w[...], preferred_element_type=F32)
    col = lax.broadcasted_iota(jnp.int32, logits.shape, 1)
    real = col < classes
    top = jnp.max(jnp.where(real, logits, -jnp.inf), axis=1, keepdims=True)
    shifted = logits - top
    log_sum = jnp.log(jnp.sum(jnp.where(real, jnp.exp(shifted), 0.0), axis=1, keepdims=True))
    log_prob = shifted - log_sum
    tag = label[...]
    hit = col == tag
    loss_sum[...] += jnp.sum(jnp.where(hit, log_prob, 0.0), axis=0, keepdims=True)
    scale = jnp.where(tag >= 0, inv_total[0], 0.0)
    grad = jnp.where(real, (jnp.exp(log_prob) - jnp.where(hit, 1.0, 0.0)) * scale, 0.0).astype(BF16)
    g_out[...] = grad
    gw_out[...] += lax.dot_general(grad, z, (((0,), (0,)), ((), ())), preferred_element_type=F32)

    @pl.when(g == pl.num_programs(0) - 1)
    def _():
        total = jnp.sum(loss_sum[...], axis=1, keepdims=True)
        gw_out[pl.ds(gw_out.shape[0] - 1, 1), pl.ds(0, LANES)] = jnp.broadcast_to(total, (1, LANES))


def scatter_kernel(src, wt, grad, s_out, gbuf, wbuf, *parts):
    g = pl.program_id(0)
    rows, deg = grad.shape[0], wt.shape[1]
    steps = rows // STEP

    @pl.when(g == 0)
    def _():
        def clear(i, carry):
            for part in parts:
                for j in range(8):
                    part[pl.ds(pl.multiple_of(i * 64, 64) + j * 8, 8), :] = jnp.zeros((8, LANES), F32)
            return carry

        lax.fori_loop(0, s_out.shape[0] // 64, clear, 0)

    x = grad[...].astype(F32)
    for c in range(2):
        gbuf[pl.ds(c, rows, stride=2), :] = x[:, c * LANES : (c + 1) * LANES]

    def weights_at(i):
        return spread_weights(wt[pl.ds(pl.multiple_of(i * STEP, STEP), STEP), :], deg)

    def step(i, tiles):
        for t, tile in enumerate(tiles):
            wbuf[pl.ds(t * 8, 8), :] = tile
        ahead = weights_at(jnp.minimum(i + 1, steps - 1))
        here = gbuf.at[pl.ds(pl.multiple_of(i * STEP * 2, STEP * 2), STEP * 2)]
        for u in range(STEP):
            row = here[pl.ds(u * 2, 2), :]
            for k in range(deg):
                at = pl.ds(pl.multiple_of(src[u * deg + k, g * steps + i], 2), 2)
                w = wbuf[pl.ds((u // 8 * deg + k) * 8 + u % 8, 2, stride=0), :]
                parts[k][at, :] = parts[k][at, :] + row * w
        return ahead

    lax.fori_loop(0, steps, step, weights_at(0))

    @pl.when(g == pl.num_programs(0) - 1)
    def _():
        def add(i, carry):
            at = pl.ds(pl.multiple_of(i * 64, 64), 64)
            total = parts[0][at, :]
            for part in parts[1:]:
                total = total + part[at, :]
            s_out[at, :] = total
            return carry

        lax.fori_loop(0, s_out.shape[0] // 64, add, 0)


def backward_kernel(lists, own, back, w_t, gw_two, h, z, gw_out, total):
    g = pl.program_id(0)
    rows = h.shape[0]

    @pl.when(g == 0)
    def _():
        f_in = z.shape[1]
        gw_out[pl.ds(0, f_in), :] = jnp.zeros((f_in, gw_out.shape[1]), F32)
        gw_out[pl.ds(f_in, gw_two.shape[0]), :] = gw_two[...]

        def copy(i, carry):
            at = pl.ds(pl.multiple_of(i * 64, 64), 64)
            total[at, :] = own[at, :]
            return carry

        lax.fori_loop(0, own.shape[0] // 64, copy, 0)

        def add(i, carry):
            for j in range(4):
                at = pl.ds(pl.multiple_of(lists[i * 4 + j], 2), 2)
                total[at, :] = total[at, :] + back[pl.ds(pl.multiple_of(i * 8, 8) + j * 2, 2), :]
            return carry

        lax.fori_loop(0, back.shape[0] // 8, add, 0)

    s = jnp.concatenate([total[pl.ds(g * rows * 2 + c, rows, stride=2), :] for c in range(2)], axis=1)
    high = s.astype(BF16)
    rest = s - high.astype(F32)
    mid = rest.astype(BF16)
    low = (rest - mid.astype(F32)).astype(BF16)
    wt = w_t[...]
    d = jnp.dot(low, wt, preferred_element_type=F32)
    d = d + jnp.dot(mid, wt, preferred_element_type=F32)
    d = d + jnp.dot(high, wt, preferred_element_type=F32)
    grad = jnp.where(h[...] > 0, d, 0.0).astype(BF16)
    gw_out[pl.ds(0, z.shape[1]), :] += lax.dot_general(z[...], grad, (((0,), (0,)), ((), ())), preferred_element_type=F32)


MESH = pl.DeviceIdType.MESH
SIDE = 4
COLORS = ((0, 384, (0, 1, 2)), (384, 384, (1, 2, 0)), (768, 256, (2, 0, 1)))


def reduce_kernel(x, out, acc, pair_buf, far, mid, near, *sems):
    pair_send, pair_recv, rs_send, rs_recv, ag_send, ag_recv, back_send, back_recv = sems
    me = lax.axis_index("graph")
    core = lax.rem(me, 2)
    where = [lax.rem(me // (2 * SIDE**d), SIDE) for d in range(3)]
    partner = me + 1 - 2 * core

    def peer(axis, t):
        p = lax.rem(where[axis] + t, SIDE)
        return p, me + (p - where[axis]) * (2 * SIDE**axis)

    barrier = pltpu.get_barrier_semaphore()
    pl.semaphore_signal(barrier, inc=1, device_id=(partner,), device_id_type=MESH)
    for axis in range(3):
        for t in range(1, SIDE):
            pl.semaphore_signal(barrier, inc=1, device_id=(peer(axis, t)[1],), device_id_type=MESH)
    pl.semaphore_wait(barrier, 10)

    def remote(src, dst, send, recv, dev):
        return pltpu.make_async_remote_copy(src_ref=src, dst_ref=dst, send_sem=send, recv_sem=recv, device_id=(dev,), device_id_type=MESH)

    pending = []
    base = pl.multiple_of(core * 512, 512)
    other = pl.multiple_of(512 - core * 512, 512)
    order = (2, 1, 3, 0)
    pair = {}
    for t in order:
        for c, (lane, width, axes) in enumerate(COLORS):
            p = lax.rem(where[axes[0]] + t, SIDE)
            rows = pl.ds(pl.multiple_of(p * 128, 128), 128)
            copy = remote(x.at[pl.ds(pl.multiple_of(other + p * 128, 128), 128), pl.ds(lane, width)], pair_buf.at[rows, pl.ds(lane, width)], pair_send.at[c, t], pair_recv.at[c, t], partner)
            copy.start()
            pair[c, t] = copy
            pending.append(copy)
    first = {}
    for t in order:
        for c, (lane, width, axes) in enumerate(COLORS):
            p, dev = peer(axes[0], t)
            rows = pl.ds(pl.multiple_of(p * 128, 128), 128)
            lanes = pl.ds(lane, width)
            pair[c, t].wait_recv()
            acc[rows, lanes] = x[pl.ds(pl.multiple_of(base + p * 128, 128), 128), lanes] + pair_buf[rows, lanes]
            if t:
                copy = remote(acc.at[rows, lanes], far.at[t - 1, :, lanes], rs_send.at[0, c, t - 1], rs_recv.at[0, c, t - 1], dev)
                copy.start()
                first[c, t] = copy
                pending.append(copy)
    start = [0, 0, 0]
    for stage, (size, buf) in enumerate(((128, far), (32, mid), (8, near))):
        if stage:
            first = {}
            for c, (lane, width, axes) in enumerate(COLORS):
                for t in (2, 1, 3):
                    p, dev = peer(axes[stage], t)
                    rows = pl.ds(pl.multiple_of(start[c] + p * size, 8), size)
                    copy = remote(acc.at[rows, pl.ds(lane, width)], buf.at[t - 1, :, pl.ds(lane, width)], rs_send.at[stage, c, t - 1], rs_recv.at[stage, c, t - 1], dev)
                    copy.start()
                    first[c, t] = copy
                    pending.append(copy)
        for c, (lane, width, axes) in enumerate(COLORS):
            lanes = pl.ds(lane, width)
            start[c] = start[c] + where[axes[stage]] * size
            rows = pl.ds(pl.multiple_of(start[c], 8), size)
            for t in (1, 2, 3):
                first[c, t].wait_recv()
            mine = acc[rows, lanes] + buf[0, :, lanes] + buf[1, :, lanes] + buf[2, :, lanes]
            if stage < 2:
                acc[rows, lanes] = mine
            else:
                out[pl.ds(pl.multiple_of(base + start[c], 8), size), lanes] = mine
    for stage, size in ((2, 8), (1, 32), (0, 128)):
        copies = {}
        for c, (lane, width, axes) in enumerate(COLORS):
            lanes = pl.ds(lane, width)
            rows = pl.ds(pl.multiple_of(base + start[c], 8), size)
            for t in (2, 1, 3):
                _, dev = peer(axes[stage], t)
                copy = remote(out.at[rows, lanes], out.at[rows, lanes], ag_send.at[stage, c, t - 1], ag_recv.at[stage, c, t - 1], dev)
                copy.start()
                copies[c, t] = copy
                pending.append(copy)
            if stage == 0:
                copy = remote(out.at[rows, lanes], out.at[rows, lanes], back_send.at[c, 0], back_recv.at[c, 0], partner)
                copy.start()
                copies[c, 0] = copy
                pending.append(copy)
        if stage:
            for c, (lane, width, axes) in enumerate(COLORS):
                for t in (1, 2, 3):
                    copies[c, t].wait_recv()
                start[c] = start[c] - where[axes[stage]] * size
        else:
            for t in (1, 3, 2):
                for c, (lane, width, axes) in enumerate(COLORS):
                    lanes = pl.ds(lane, width)
                    copies[c, t].wait_recv()
                    p, _ = peer(axes[0], SIDE - t)
                    rows = pl.ds(pl.multiple_of(base + p * 128, 128), 128)
                    copy = remote(out.at[rows, lanes], out.at[rows, lanes], back_send.at[c, t], back_recv.at[c, t], partner)
                    copy.start()
                    copies[c, t + 4] = copy
                    pending.append(copy)
            for c in range(3):
                copies[c, 0].wait_recv()
                for t in (1, 2, 3):
                    copies[c, t + 4].wait_recv()
    for copy in pending:
        copy.wait_send()


def reduce_all(x):
    sem = pltpu.SemaphoreType.DMA
    return pl.pallas_call(reduce_kernel,
        in_specs=[pl.BlockSpec(memory_space=pltpu.VMEM)], out_specs=pl.BlockSpec(memory_space=pltpu.VMEM),
        out_shape=jax.ShapeDtypeStruct((1024,1024),F32),
        scratch_shapes=[pltpu.VMEM((512,1024),F32), pltpu.VMEM((512,1024),F32), pltpu.VMEM((3,128,1024),F32), pltpu.VMEM((3,32,1024),F32), pltpu.VMEM((3,8,1024),F32),
            sem((3,4)), sem((3,4)), sem((3,3,3)), sem((3,3,3)), sem((3,3,3)), sem((3,3,3)), sem((3,4)), sem((3,4))],
        compiler_params=pltpu.CompilerParams(collective_id=0, has_side_effects=True, vmem_limit_bytes=40*2**20),
        name="reduce_all")(x)


def exchange_body(n, outs, ins, sems):
    me = lax.axis_index("graph")

    def send(t, carry):
        q = lax.rem(me + t, n)
        for j, (o, i) in enumerate(zip(outs, ins)):
            src = o.at[q] if o.shape[0] == n else o.at[0]
            pltpu.make_async_remote_copy(src_ref=src, dst_ref=i.at[me], send_sem=sems[2*j], recv_sem=sems[2*j+1], device_id=(q,), device_id_type=MESH).start()
        return carry
    lax.fori_loop(1, n, send, 0)
    for j, (o, i) in enumerate(zip(outs, ins)):
        whole = i.at[pl.ds(0, n - 1)]
        pltpu.make_async_copy(whole, whole, sems[2*j]).wait()
        pltpu.make_async_copy(whole, whole, sems[2*j+1]).wait()

def exchange(n, *arrays, name="exchange"):
    k = len(arrays)
    def kernel(*refs):
        exchange_body(n, refs[:k], refs[k:2*k], refs[2*k:])
    return pl.pallas_call(kernel,
        in_specs=[pl.BlockSpec(memory_space=pltpu.VMEM)]*k, out_specs=[pl.BlockSpec(memory_space=pltpu.VMEM)]*k,
        out_shape=[jax.ShapeDtypeStruct((n,)+a.shape[1:], a.dtype) for a in arrays],
        scratch_shapes=[pltpu.SemaphoreType.DMA]*(2*k),
        compiler_params=pltpu.CompilerParams(has_side_effects=True, vmem_limit_bytes=40*2**20),
        name=name)(*arrays)


def params():
    return pltpu.CompilerParams(dimension_semantics=("arbitrary",), vmem_limit_bytes=62 * 2**20)


SMEM = pl.BlockSpec(memory_space=pltpu.SMEM)


def solution(mesh):
    dev_count = mesh.shape["graph"]

    def device_step(feats, w_one, w_two, send_idx, send_count, edge_src, edge_wt, labels, label_mask):
        n, f_in = feats.shape
        f_hid, classes = w_two.shape
        halo_rows, deg = send_idx.shape[1], edge_src.shape[1]
        halo = dev_count * halo_rows
        ext = n + halo
        pad = 2 * LANES
        w_one_b = w_one.astype(BF16)
        w_two_b = jnp.pad(w_two.astype(BF16), ((0, 0), (0, pad - classes)))
        list_ids = send_idx.reshape(halo)
        list_ok = jnp.arange(halo_rows)[None, :] < send_count[:, None]
        src_t = edge_src.reshape(n // STEP, STEP * deg).T
        src8, src2 = src_t * 8, src_t * 2
        lists2 = jnp.where(list_ok, send_idx, n).reshape(halo) * 2
        label = jnp.where(label_mask == 1, labels, -1).reshape(n, 1)
        ok_rows = list_ok.reshape(halo, 1)
        count = jnp.sum(label_mask.astype(F32))
        first_rows = jnp.where(ok_rows, feats[list_ids], 0).reshape(dev_count, halo_rows, f_in)
        feats_in, counts = exchange(dev_count, first_rows, jnp.full((1, 1, LANES), count), name="exchange_one")
        mine = jnp.arange(dev_count) == lax.axis_index("graph")
        label_total = jnp.sum(jnp.where(mine, count, counts[:, 0, 0]))
        inv_total = (1.0 / label_total).reshape(1)

        def by_rows(width):
            return pl.BlockSpec((BLOCK, width), lambda g: (g, 0))

        gather_scratch = [
            pltpu.VMEM((ext * 8, LANES), F32),
            pltpu.VMEM((BLOCK * 8, LANES), F32),
            pltpu.VMEM((STEP * deg + 8, LANES), F32),
        ]
        z_one, h_one = pl.pallas_call(
            layer_one_kernel,
            grid=(n // BLOCK,),
            in_specs=[SMEM, by_rows(deg), once((n, f_in)), once((halo, f_in)), once((f_in, f_hid))],
            out_specs=[by_rows(f_in), by_rows(f_hid)],
            out_shape=[jax.ShapeDtypeStruct((n, f_in), BF16), jax.ShapeDtypeStruct((n, f_hid), BF16)],
            scratch_shapes=gather_scratch,
            compiler_params=params(),
            name="layer_one",
        )(src8, edge_wt, feats, feats_in.reshape(halo, f_in), w_one_b)
        second_rows = jnp.where(ok_rows, h_one[list_ids], 0)
        h_in = lax.all_to_all(second_rows, "graph", 0, 0, tiled=True)
        grad_log, gw_two = pl.pallas_call(
            functools.partial(layer_two_kernel, classes),
            grid=(n // BLOCK,),
            in_specs=[SMEM, SMEM, by_rows(deg), once((n, f_hid)), once((halo, f_hid)), once((f_hid, pad)), by_rows(1)],
            out_specs=[by_rows(pad), once((pad, f_hid))],
            out_shape=[jax.ShapeDtypeStruct((n, pad), BF16), jax.ShapeDtypeStruct((pad, f_hid), F32)],
            scratch_shapes=gather_scratch + [pltpu.VMEM((1, pad), F32)],
            compiler_params=params(),
            name="layer_two",
        )(src8, inv_total, edge_wt, h_one, h_in, w_two_b, label)
        ext_grad = pl.pallas_call(
            scatter_kernel,
            grid=(n // 512,),
            in_specs=[SMEM, pl.BlockSpec((512, deg), lambda g: (g, 0)), pl.BlockSpec((512, pad), lambda g: (g, 0))],
            out_specs=once((ext * 2, LANES)),
            out_shape=jax.ShapeDtypeStruct((ext * 2, LANES), F32),
            scratch_shapes=[pltpu.VMEM((512 * 2, LANES), F32), pltpu.VMEM((STEP * deg + 8, LANES), F32)]
            + [pltpu.VMEM((ext * 2, LANES), F32) for _ in range(deg)],
            compiler_params=params(),
            name="scatter",
        )(src2, edge_wt, grad_log)
        back = lax.all_to_all(ext_grad[n * 2 :], "graph", 0, 0, tiled=True)
        partial = pl.pallas_call(
            backward_kernel,
            grid=(n // 512,),
            in_specs=[
                SMEM,
                once((n * 2, LANES)),
                once((halo * 2, LANES)),
                once((pad, f_hid)),
                once((pad, f_hid)),
                pl.BlockSpec((512, f_hid), lambda g: (g, 0)),
                pl.BlockSpec((512, f_in), lambda g: (g, 0)),
            ],
            out_specs=once((f_in + pad, f_hid)),
            out_shape=jax.ShapeDtypeStruct((f_in + pad, f_hid), F32),
            scratch_shapes=[pltpu.VMEM((n * 2 + 8, LANES), F32)],
            compiler_params=params(),
            name="backward",
        )(lists2, ext_grad, back, w_two_b.T, gw_two, h_one, z_one)
        total = reduce_all(partial)
        return -total[f_in + pad - 1, 0] / label_total, total[:f_in], total[f_in : f_in + classes].T

    row_spec = P("graph", None)
    vec_spec = P("graph")
    return jax.shard_map(
        device_step,
        mesh=mesh,
        in_specs=(row_spec, P(), P(), row_spec, vec_spec, row_spec, row_spec, vec_spec, vec_spec),
        out_specs=(P(), P(), P()),
        check_vma=False,
    )
```

```python
import functools

import jax
import jax.numpy as jnp
from jax import lax
from jax.experimental import pallas as pl
from jax.experimental.pallas import tpu as pltpu
from jax.sharding import PartitionSpec as P

LANES = 128
STEP = 16
BLOCK = 512
F32, BF16 = jnp.float32, jnp.bfloat16


def once(shape):
    return pl.BlockSpec(shape, lambda g: (0,) * len(shape), pipeline_mode=pl.Buffered(1))


def fill_rows(dst, src, offset, blocks):
    def step(i, carry):
        r = pl.multiple_of(i * 64, 64)
        x = src[pl.ds(r, 64), :].astype(F32)
        for c in range(blocks):
            dst[pl.ds((r + offset) * 8 + c, 64, stride=8), :] = x[:, c * LANES : (c + 1) * LANES]
        return carry

    lax.fori_loop(0, src.shape[0] // 64, step, 0)


def put_weights(wbuf, w):
    deg = w.shape[1]
    for h in range(STEP // 8):
        for k in range(deg):
            tile = jnp.broadcast_to(w[h * 8 : h * 8 + 8, k : k + 1], (8, LANES))
            wbuf[pl.ds((h * deg + k) * 8, 8), :] = tile


def gather_rows(steps, row_of, src, wt, table, out, wbuf):
    deg = wt.shape[1]

    def put(i):
        put_weights(wbuf, wt[pl.ds(pl.multiple_of(i * STEP, STEP), STEP), :])

    put(0)

    def step(i, carry):
        dst = out.at[pl.ds(pl.multiple_of(i * STEP * 8, STEP * 8), STEP * 8)]
        for u in range(STEP):
            n = row_of(i * STEP + u)
            acc = None
            for k in range(deg):
                row = table[pl.ds(pl.multiple_of(src[k][n], 8), 8), :]
                term = row * wbuf[pl.ds((u // 8 * deg + k) * 8 + u % 8, 8, stride=0), :]
                acc = term if acc is None else acc + term
            dst[pl.ds(u * 8, 8), :] = acc
        put(jnp.minimum(i + 1, steps - 1))
        return carry

    lax.fori_loop(0, steps, step, 0)


def load_sources(src_hbm, src, sems):
    n = src[0].shape[0]
    copies = [pltpu.make_async_copy(src_hbm.at[pl.ds(k * n, n)], ref, sems.at[k]) for k, ref in enumerate(src)]
    for copy in copies:
        copy.start()
    return copies


def fill_tiles(dst, src, offset):
    def step(i, carry):
        at = pl.multiple_of(i * 128, 128)
        dst[pl.ds(pl.multiple_of(offset * 8 + at, 8), 128), :] = src[pl.ds(at, 128), :].astype(F32)
        return carry

    lax.fori_loop(0, src.shape[0] // 128, step, 0)


def layer_one_kernel(lists, list_ok, src_hbm, feats, halo, wt_t, w_f32, z_out, h_out, wt_out, second,
                     table, zbuf, wbuf, w, chunk, list_wt, src_sem, chunk_sem, *src):
    g = pl.program_id(0)
    rows, blocks = z_out.shape[0], feats.shape[1] // LANES
    n, deg = wt_out.shape

    def aggregate():
        return jnp.concatenate([zbuf[pl.ds(c, rows, stride=8), :] for c in range(blocks)], axis=1).astype(BF16)

    def hidden(z):
        return jnp.maximum(jnp.dot(z, w[...], preferred_element_type=F32), 0.0)

    @pl.when(g == 0)
    def _():
        index_copies = load_sources(src_hbm, src, src_sem)

        def fetch(i):
            slot = lax.rem(i, 2)
            return pltpu.make_async_copy(feats.at[pl.ds(pl.multiple_of(i * rows, rows), rows), :], chunk.at[slot], chunk_sem.at[slot])

        fetch(0).start()

        def turn(i, carry):
            at = pl.ds(pl.multiple_of(i * LANES, LANES), LANES)
            wt_out[at, :] = wt_t[:, at].T
            return carry

        lax.fori_loop(0, n // LANES, turn, 0)
        w[...] = w_f32[...].astype(BF16)
        fill_rows(table, halo, n, blocks)

        def take(i, carry):
            @pl.when(i + 1 < n // rows)
            def _():
                fetch(i + 1).start()

            fetch(i).wait()
            slot = lax.rem(i, 2)

            def fill(j, carry):
                r = pl.multiple_of(j * 64, 64)
                x = chunk[slot, pl.ds(r, 64), :].astype(F32)
                for c in range(blocks):
                    table[pl.ds((i * rows + r) * 8 + c, 64, stride=8), :] = x[:, c * LANES : (c + 1) * LANES]
                return carry

            return lax.fori_loop(0, rows // 64, fill, carry)

        lax.fori_loop(0, n // rows, take, 0)

        def pick(i, carry):
            for u in range(8):
                j = i * 8 + u
                list_wt[pl.ds(j, 1), :] = wt_out[pl.ds(lists[j], 1), :] * list_ok[j]
            return carry

        lax.fori_loop(0, rows // 8, pick, 0)
        for copy in index_copies:
            copy.wait()
        gather_rows(rows // STEP, lambda j: lists[j], src, list_wt, table, zbuf, wbuf)
        h = hidden(aggregate())
        for c in range(h.shape[1] // LANES):
            zbuf[pl.ds(c, rows, stride=8), :] = h[:, c * LANES : (c + 1) * LANES]
        second[...] = zbuf[...].astype(BF16)

    @pl.when(g > 0)
    def _():
        first_row = pl.multiple_of((g - 1) * rows, rows)
        gather_rows(rows // STEP, lambda j: first_row + j, src, wt_out.at[pl.ds(first_row, rows)], table, zbuf, wbuf)
        z = aggregate()
        z_out[...] = z
        h_out[...] = hidden(z).astype(BF16)


def layer_two_kernel(classes, src_hbm, inv_total, wt, own, halo, w, label, g_out, gw_out, table, zbuf, wbuf, loss_sum, src_sem, *src):
    g = pl.program_id(0)
    rows, blocks = g_out.shape[0], own.shape[1] // LANES

    @pl.when(g == 0)
    def _():
        index_copies = load_sources(src_hbm, src, src_sem)
        fill_rows(table, own, 0, blocks)
        fill_tiles(table, halo, own.shape[0])
        for copy in index_copies:
            copy.wait()
        gw_out[...] = jnp.zeros_like(gw_out)
        loss_sum[...] = jnp.zeros_like(loss_sum)

    first_row = g * rows
    gather_rows(rows // STEP, lambda j: first_row + j, src, wt, table, zbuf, wbuf)
    z = jnp.concatenate([zbuf[pl.ds(c, rows, stride=8), :] for c in range(blocks)], axis=1).astype(BF16)
    logits = jnp.dot(z, w[...], preferred_element_type=F32)
    col = lax.broadcasted_iota(jnp.int32, logits.shape, 1)
    real = col < classes
    top = jnp.max(jnp.where(real, logits, -jnp.inf), axis=1, keepdims=True)
    shifted = logits - top
    log_sum = jnp.log(jnp.sum(jnp.where(real, jnp.exp(shifted), 0.0), axis=1, keepdims=True))
    log_prob = shifted - log_sum
    tag = label[...]
    hit = col == tag
    loss_sum[...] += jnp.sum(jnp.where(hit, log_prob, 0.0), axis=0, keepdims=True)
    scale = jnp.where(tag >= 0, inv_total[0], 0.0)
    grad = jnp.where(real, (jnp.exp(log_prob) - jnp.where(hit, 1.0, 0.0)) * scale, 0.0).astype(BF16)
    g_out[...] = grad
    gw_out[...] += lax.dot_general(grad, z, (((0,), (0,)), ((), ())), preferred_element_type=F32)

    @pl.when(g == pl.num_programs(0) - 1)
    def _():
        total = jnp.sum(loss_sum[...], axis=1, keepdims=True)
        gw_out[pl.ds(gw_out.shape[0] - 1, 1), pl.ds(0, LANES)] = jnp.broadcast_to(total, (1, LANES))


def scatter_kernel(src_hbm, wt, grad, s_out, gbuf, wbuf, src_sem, *refs):
    g = pl.program_id(0)
    rows, deg = grad.shape[0], wt.shape[1]
    src, parts = refs[:deg], refs[deg:]
    steps = rows // STEP

    @pl.when(g == 0)
    def _():
        index_copies = load_sources(src_hbm, src, src_sem)

        def clear(i, carry):
            for part in parts:
                for j in range(8):
                    part[pl.ds(pl.multiple_of(i * 64, 64) + j * 8, 8), :] = jnp.zeros((8, LANES), F32)
            return carry

        lax.fori_loop(0, s_out.shape[0] // 64, clear, 0)
        for copy in index_copies:
            copy.wait()

    x = grad[...].astype(F32)
    for c in range(2):
        gbuf[pl.ds(c, rows, stride=2), :] = x[:, c * LANES : (c + 1) * LANES]

    def put(i):
        put_weights(wbuf, wt[pl.ds(pl.multiple_of(i * STEP, STEP), STEP), :])

    put(0)

    def step(i, carry):
        here = gbuf.at[pl.ds(pl.multiple_of(i * STEP * 2, STEP * 2), STEP * 2)]
        for u in range(STEP):
            row = here[pl.ds(u * 2, 2), :]
            n = g * rows + i * STEP + u
            for k in range(deg):
                at = pl.ds(pl.multiple_of(src[k][n], 2), 2)
                w = wbuf[pl.ds((u // 8 * deg + k) * 8 + u % 8, 2, stride=0), :]
                parts[k][at, :] = parts[k][at, :] + row * w
        put(jnp.minimum(i + 1, steps - 1))
        return carry

    lax.fori_loop(0, steps, step, 0)

    @pl.when(g == pl.num_programs(0) - 1)
    def _():
        def add(i, carry):
            at = pl.ds(pl.multiple_of(i * 64, 64), 64)
            total = parts[0][at, :]
            for part in parts[1:]:
                total = total + part[at, :]
            s_out[at, :] = total
            return carry

        lax.fori_loop(0, s_out.shape[0] // 64, add, 0)


def backward_kernel(lists, own, back, w_t, gw_two, h, z, gw_out, total):
    g = pl.program_id(0)
    rows = h.shape[0]

    @pl.when(g == 0)
    def _():
        f_in = z.shape[1]
        gw_out[pl.ds(0, f_in), :] = jnp.zeros((f_in, gw_out.shape[1]), F32)
        gw_out[pl.ds(f_in, gw_two.shape[0]), :] = gw_two[...]

        def copy(i, carry):
            at = pl.ds(pl.multiple_of(i * 64, 64), 64)
            total[at, :] = own[at, :]
            return carry

        lax.fori_loop(0, own.shape[0] // 64, copy, 0)

        def add(i, carry):
            for j in range(4):
                at = pl.ds(pl.multiple_of(lists[i * 4 + j], 2), 2)
                total[at, :] = total[at, :] + back[pl.ds(pl.multiple_of(i * 8, 8) + j * 2, 2), :]
            return carry

        lax.fori_loop(0, back.shape[0] // 8, add, 0)

    s = jnp.concatenate([total[pl.ds(g * rows * 2 + c, rows, stride=2), :] for c in range(2)], axis=1)
    high = s.astype(BF16)
    rest = s - high.astype(F32)
    mid = rest.astype(BF16)
    low = (rest - mid.astype(F32)).astype(BF16)
    wt = w_t[...]
    d = jnp.dot(low, wt, preferred_element_type=F32)
    d = d + jnp.dot(mid, wt, preferred_element_type=F32)
    d = d + jnp.dot(high, wt, preferred_element_type=F32)
    grad = jnp.where(h[...] > 0, d, 0.0).astype(BF16)
    gw_out[pl.ds(0, z.shape[1]), :] += lax.dot_general(z[...], grad, (((0,), (0,)), ((), ())), preferred_element_type=F32)


MESH = pl.DeviceIdType.MESH
SIDE = 4
COLORS = ((0, 384, (0, 1, 2)), (384, 384, (1, 2, 0)), (768, 256, (2, 0, 1)))


def reduce_kernel(x, out, acc, pair_buf, far, mid, near, *sems):
    pair_send, pair_recv, rs_send, rs_recv, ag_send, ag_recv, back_send, back_recv = sems
    me = lax.axis_index("graph")
    core = lax.rem(me, 2)
    where = [lax.rem(me // (2 * SIDE**d), SIDE) for d in range(3)]
    partner = me + 1 - 2 * core

    def peer(axis, t):
        p = lax.rem(where[axis] + t, SIDE)
        return p, me + (p - where[axis]) * (2 * SIDE**axis)

    barrier = pltpu.get_barrier_semaphore()
    pl.semaphore_signal(barrier, inc=1, device_id=(partner,), device_id_type=MESH)
    for axis in range(3):
        for t in range(1, SIDE):
            pl.semaphore_signal(barrier, inc=1, device_id=(peer(axis, t)[1],), device_id_type=MESH)
    pl.semaphore_wait(barrier, 10)

    def remote(src, dst, send, recv, dev):
        return pltpu.make_async_remote_copy(src_ref=src, dst_ref=dst, send_sem=send, recv_sem=recv, device_id=(dev,), device_id_type=MESH)

    pending = []
    base = pl.multiple_of(core * 512, 512)
    other = pl.multiple_of(512 - core * 512, 512)
    order = (2, 1, 3, 0)
    pair = {}
    for t in order:
        for c, (lane, width, axes) in enumerate(COLORS):
            p = lax.rem(where[axes[0]] + t, SIDE)
            rows = pl.ds(pl.multiple_of(p * 128, 128), 128)
            copy = remote(x.at[pl.ds(pl.multiple_of(other + p * 128, 128), 128), pl.ds(lane, width)], pair_buf.at[rows, pl.ds(lane, width)], pair_send.at[c, t], pair_recv.at[c, t], partner)
            copy.start()
            pair[c, t] = copy
            pending.append(copy)
    first = {}
    for t in order:
        for c, (lane, width, axes) in enumerate(COLORS):
            p, dev = peer(axes[0], t)
            rows = pl.ds(pl.multiple_of(p * 128, 128), 128)
            lanes = pl.ds(lane, width)
            pair[c, t].wait_recv()
            acc[rows, lanes] = x[pl.ds(pl.multiple_of(base + p * 128, 128), 128), lanes] + pair_buf[rows, lanes]
            if t:
                copy = remote(acc.at[rows, lanes], far.at[t - 1, :, lanes], rs_send.at[0, c, t - 1], rs_recv.at[0, c, t - 1], dev)
                copy.start()
                first[c, t] = copy
                pending.append(copy)
    start = [0, 0, 0]
    for stage, (size, buf) in enumerate(((128, far), (32, mid), (8, near))):
        if stage:
            first = {}
            for c, (lane, width, axes) in enumerate(COLORS):
                for t in (2, 1, 3):
                    p, dev = peer(axes[stage], t)
                    rows = pl.ds(pl.multiple_of(start[c] + p * size, 8), size)
                    copy = remote(acc.at[rows, pl.ds(lane, width)], buf.at[t - 1, :, pl.ds(lane, width)], rs_send.at[stage, c, t - 1], rs_recv.at[stage, c, t - 1], dev)
                    copy.start()
                    first[c, t] = copy
                    pending.append(copy)
        for c, (lane, width, axes) in enumerate(COLORS):
            lanes = pl.ds(lane, width)
            start[c] = start[c] + where[axes[stage]] * size
            rows = pl.ds(pl.multiple_of(start[c], 8), size)
            for t in (1, 2, 3):
                first[c, t].wait_recv()
            mine = acc[rows, lanes] + buf[0, :, lanes] + buf[1, :, lanes] + buf[2, :, lanes]
            if stage < 2:
                acc[rows, lanes] = mine
            else:
                out[pl.ds(pl.multiple_of(base + start[c], 8), size), lanes] = mine
    for stage, size in ((2, 8), (1, 32), (0, 128)):
        copies = {}
        for c, (lane, width, axes) in enumerate(COLORS):
            lanes = pl.ds(lane, width)
            rows = pl.ds(pl.multiple_of(base + start[c], 8), size)
            for t in (2, 1, 3):
                _, dev = peer(axes[stage], t)
                copy = remote(out.at[rows, lanes], out.at[rows, lanes], ag_send.at[stage, c, t - 1], ag_recv.at[stage, c, t - 1], dev)
                copy.start()
                copies[c, t] = copy
                pending.append(copy)
            if stage == 0:
                copy = remote(out.at[rows, lanes], out.at[rows, lanes], back_send.at[c, 0], back_recv.at[c, 0], partner)
                copy.start()
                copies[c, 0] = copy
                pending.append(copy)
        if stage:
            for c, (lane, width, axes) in enumerate(COLORS):
                for t in (1, 2, 3):
                    copies[c, t].wait_recv()
                start[c] = start[c] - where[axes[stage]] * size
        else:
            for t in (1, 3, 2):
                for c, (lane, width, axes) in enumerate(COLORS):
                    lanes = pl.ds(lane, width)
                    copies[c, t].wait_recv()
                    p, _ = peer(axes[0], SIDE - t)
                    rows = pl.ds(pl.multiple_of(base + p * 128, 128), 128)
                    copy = remote(out.at[rows, lanes], out.at[rows, lanes], back_send.at[c, t], back_recv.at[c, t], partner)
                    copy.start()
                    copies[c, t + 4] = copy
                    pending.append(copy)
            for c in range(3):
                copies[c, 0].wait_recv()
                for t in (1, 2, 3):
                    copies[c, t + 4].wait_recv()
    for copy in pending:
        copy.wait_send()


def reduce_all(x):
    sem = pltpu.SemaphoreType.DMA
    return pl.pallas_call(reduce_kernel,
        in_specs=[pl.BlockSpec(memory_space=pltpu.VMEM)], out_specs=pl.BlockSpec(memory_space=pltpu.VMEM),
        out_shape=jax.ShapeDtypeStruct((1024,1024),F32),
        scratch_shapes=[pltpu.VMEM((512,1024),F32), pltpu.VMEM((512,1024),F32), pltpu.VMEM((3,128,1024),F32), pltpu.VMEM((3,32,1024),F32), pltpu.VMEM((3,8,1024),F32),
            sem((3,4)), sem((3,4)), sem((3,3,3)), sem((3,3,3)), sem((3,3,3)), sem((3,3,3)), sem((3,4)), sem((3,4))],
        compiler_params=pltpu.CompilerParams(collective_id=0, has_side_effects=True, vmem_limit_bytes=40*2**20),
        name="reduce_all")(x)


def count_kernel(x, out, came, send, recv):
    me = lax.axis_index("graph")
    hops = [(1, 2)] + [(2 * SIDE**axis, SIDE) for axis in range(3)]

    def peer(stride, size, t):
        here = lax.rem(me // stride, size)
        return me + (lax.rem(here + t, size) - here) * stride

    barrier = pltpu.get_barrier_semaphore()
    for stride, size in hops:
        for t in range(1, size):
            pl.semaphore_signal(barrier, inc=1, device_id=(peer(stride, size, t),), device_id_type=MESH)
    pl.semaphore_wait(barrier, came.shape[0])
    out[0] = x[...]
    slot = 0
    copies = []
    for stage, (stride, size) in enumerate(hops):
        step = []
        for t in range(1, size):
            at = slot + t - 1
            step.append(
                pltpu.make_async_remote_copy(
                    src_ref=out.at[stage],
                    dst_ref=came.at[at],
                    send_sem=send.at[at],
                    recv_sem=recv.at[at],
                    device_id=(peer(stride, size, t),),
                    device_id_type=MESH,
                )
            )
            step[-1].start()
        total = out[stage]
        for t, copy in enumerate(step):
            copy.wait_recv()
            total = total + came[slot + t]
        out[stage + 1] = total
        slot += size - 1
        copies += step
    for copy in copies:
        copy.wait_send()


def count_all(x):
    vmem = pl.BlockSpec(memory_space=pltpu.VMEM)
    return pl.pallas_call(
        count_kernel,
        in_specs=[vmem],
        out_specs=vmem,
        out_shape=jax.ShapeDtypeStruct((5, 8, LANES), F32),
        scratch_shapes=[pltpu.VMEM((10, 8, LANES), F32), pltpu.SemaphoreType.DMA((10,)), pltpu.SemaphoreType.DMA((10,))],
        compiler_params=pltpu.CompilerParams(collective_id=1, has_side_effects=True, vmem_limit_bytes=2**20),
        name="count_all",
    )(x)


def params():
    return pltpu.CompilerParams(dimension_semantics=("arbitrary",), vmem_limit_bytes=62 * 2**20)


SMEM = pl.BlockSpec(memory_space=pltpu.SMEM)


def solution(mesh):
    dev_count = mesh.shape["graph"]

    def device_step(feats, w_one, w_two, send_idx, send_count, edge_src, edge_wt, labels, label_mask):
        n, f_in = feats.shape
        f_hid, classes = w_two.shape
        halo_rows, deg = send_idx.shape[1], edge_src.shape[1]
        halo = dev_count * halo_rows
        ext = n + halo
        pad = 2 * LANES
        w_two_b = jnp.pad(w_two.astype(BF16), ((0, 0), (0, pad - classes)))
        list_ok = jnp.arange(halo_rows)[None, :] < send_count[:, None]
        list_ids = send_idx.reshape(halo)
        first_rows = jnp.where(list_ok.reshape(halo, 1), feats[list_ids], 0)
        first_in = lax.all_to_all(first_rows, "graph", 0, 0, tiled=True)
        lists2 = jnp.where(list_ok, send_idx, n).reshape(halo) * 2
        src_t = edge_src.T.reshape(deg * n)
        src8, src2 = src_t * 8, src_t * 2
        label = jnp.where(label_mask == 1, labels, -1).reshape(n, 1)
        count = jnp.sum(label_mask.astype(F32))

        def by_rows(width):
            return pl.BlockSpec((BLOCK, width), lambda g: (g, 0))

        def after_first(width):
            return pl.BlockSpec((BLOCK, width), lambda g: (jnp.maximum(g - 1, 0), 0))

        gather_scratch = [
            pltpu.VMEM((ext * 8, LANES), F32),
            pltpu.VMEM((BLOCK * 8, LANES), F32),
            pltpu.VMEM((STEP * deg + 8, LANES), F32),
        ]
        index_scratch = [pltpu.SMEM((n,), jnp.int32) for _ in range(deg)]
        whole = pl.BlockSpec(memory_space=pl.ANY)
        dma = pltpu.SemaphoreType.DMA
        z_one, h_one, wt, second = pl.pallas_call(
            layer_one_kernel,
            grid=(1 + n // BLOCK,),
            in_specs=[SMEM, SMEM, whole, whole, once((halo, f_in)), once((deg, n)), once((f_in, f_hid))],
            out_specs=[after_first(f_in), after_first(f_hid), once((n, deg)), once((halo * 8, LANES))],
            out_shape=[
                jax.ShapeDtypeStruct((n, f_in), BF16),
                jax.ShapeDtypeStruct((n, f_hid), BF16),
                jax.ShapeDtypeStruct((n, deg), F32),
                jax.ShapeDtypeStruct((halo * 8, LANES), BF16),
            ],
            scratch_shapes=gather_scratch
            + [
                pltpu.VMEM((f_in, f_hid), BF16),
                pltpu.VMEM((2, BLOCK, f_in), BF16),
                pltpu.VMEM((halo, deg), F32),
                dma((deg,)),
                dma((2,)),
            ]
            + index_scratch,
            compiler_params=params(),
            name="layer_one",
        )(list_ids, list_ok.reshape(halo).astype(F32), src8, feats, first_in, edge_wt.T, w_one)
        count, second = lax.optimization_barrier((count, second))
        h_in = lax.all_to_all(second, "graph", 0, 0, tiled=True)
        label_total = count_all(jnp.full((8, LANES), count))[4, 0, 0]
        inv_total = (1.0 / label_total).reshape(1)
        grad_log, gw_two = pl.pallas_call(
            functools.partial(layer_two_kernel, classes),
            grid=(n // BLOCK,),
            in_specs=[whole, SMEM, by_rows(deg), once((n, f_hid)), once((halo * 8, LANES)), once((f_hid, pad)), by_rows(1)],
            out_specs=[by_rows(pad), once((pad, f_hid))],
            out_shape=[jax.ShapeDtypeStruct((n, pad), BF16), jax.ShapeDtypeStruct((pad, f_hid), F32)],
            scratch_shapes=gather_scratch + [pltpu.VMEM((1, pad), F32), dma((deg,))] + index_scratch,
            compiler_params=params(),
            name="layer_two",
        )(src8, inv_total, wt, h_one, h_in, w_two_b, label)
        ext_grad = pl.pallas_call(
            scatter_kernel,
            grid=(n // 512,),
            in_specs=[whole, by_rows(deg), by_rows(pad)],
            out_specs=once((ext * 2, LANES)),
            out_shape=jax.ShapeDtypeStruct((ext * 2, LANES), F32),
            scratch_shapes=[pltpu.VMEM((BLOCK * 2, LANES), F32), pltpu.VMEM((STEP * deg + 8, LANES), F32), dma((deg,))]
            + index_scratch
            + [pltpu.VMEM((ext * 2, LANES), F32) for _ in range(deg)],
            compiler_params=params(),
            name="scatter",
        )(src2, wt, grad_log)
        back = lax.all_to_all(ext_grad[n * 2 :], "graph", 0, 0, tiled=True)
        partial = pl.pallas_call(
            backward_kernel,
            grid=(n // 512,),
            in_specs=[
                SMEM,
                once((n * 2, LANES)),
                once((halo * 2, LANES)),
                once((pad, f_hid)),
                once((pad, f_hid)),
                pl.BlockSpec((512, f_hid), lambda g: (g, 0)),
                pl.BlockSpec((512, f_in), lambda g: (g, 0)),
            ],
            out_specs=once((f_in + pad, f_hid)),
            out_shape=jax.ShapeDtypeStruct((f_in + pad, f_hid), F32),
            scratch_shapes=[pltpu.VMEM((n * 2 + 8, LANES), F32)],
            compiler_params=params(),
            name="backward",
        )(lists2, ext_grad, back, w_two_b.T, gw_two, h_one, z_one)
        total = reduce_all(partial)
        return -total[f_in + pad - 1, 0] / label_total, total[:f_in], total[f_in : f_in + classes].T

    row_spec = P("graph", None)
    vec_spec = P("graph")
    return jax.shard_map(
        device_step,
        mesh=mesh,
        in_specs=(row_spec, P(), P(), row_spec, vec_spec, row_spec, row_spec, vec_spec, vec_spec),
        out_specs=(P(), P(), P()),
        check_vma=False,
    )
```

```python
import functools

import jax
import jax.numpy as jnp
from jax import lax
from jax.experimental import pallas as pl
from jax.experimental.pallas import tpu as pltpu
from jax.sharding import PartitionSpec as P

LANES = 128
STEP = 16
BLOCK = 512
F32, BF16 = jnp.float32, jnp.bfloat16


def once(shape):
    return pl.BlockSpec(shape, lambda g: (0,) * len(shape), pipeline_mode=pl.Buffered(1))


def fill_rows(dst, src, offset, blocks):
    def step(i, carry):
        r = pl.multiple_of(i * 64, 64)
        x = src[pl.ds(r, 64), :].astype(F32)
        for c in range(blocks):
            dst[pl.ds((r + offset) * 8 + c, 64, stride=8), :] = x[:, c * LANES : (c + 1) * LANES]
        return carry

    lax.fori_loop(0, src.shape[0] // 64, step, 0)


def put_weights(wbuf, w):
    deg = w.shape[1]
    for h in range(STEP // 8):
        for k in range(deg):
            tile = jnp.broadcast_to(w[h * 8 : h * 8 + 8, k : k + 1], (8, LANES))
            wbuf[pl.ds((h * deg + k) * 8, 8), :] = tile


def gather_rows(steps, row_of, src, wt, table, out, wbuf):
    deg = wt.shape[1]

    def put(i):
        put_weights(wbuf, wt[pl.ds(pl.multiple_of(i * STEP, STEP), STEP), :])

    put(0)

    def step(i, carry):
        dst = out.at[pl.ds(pl.multiple_of(i * STEP * 8, STEP * 8), STEP * 8)]
        for u in range(STEP):
            n = row_of(i * STEP + u)
            acc = None
            for k in range(deg):
                row = table[pl.ds(pl.multiple_of(src[k][n], 8), 8), :]
                term = row * wbuf[pl.ds((u // 8 * deg + k) * 8 + u % 8, 8, stride=0), :]
                acc = term if acc is None else acc + term
            dst[pl.ds(u * 8, 8), :] = acc
        put(jnp.minimum(i + 1, steps - 1))
        return carry

    lax.fori_loop(0, steps, step, 0)


def fill_tiles(dst, src, offset):
    def step(i, carry):
        at = pl.multiple_of(i * 128, 128)
        dst[pl.ds(pl.multiple_of(offset * 8 + at, 8), 128), :] = src[pl.ds(at, 128), :].astype(F32)
        return carry

    lax.fori_loop(0, src.shape[0] // 128, step, 0)


def layer_one_kernel(deg, lists, *refs):
    src, (feats, halo, wt_t, w_f32, z_out, h_out, wt_out, second, table, zbuf, wbuf, w, list_wt) = refs[:deg], refs[deg:]
    g = pl.program_id(0)
    rows, blocks = z_out.shape[0], feats.shape[1] // LANES
    n = wt_out.shape[0]

    def aggregate():
        return jnp.concatenate([zbuf[pl.ds(c, rows, stride=8), :] for c in range(blocks)], axis=1).astype(BF16)

    def hidden(z):
        return jnp.maximum(jnp.dot(z, w[...], preferred_element_type=F32), 0.0)

    @pl.when(g == 0)
    def _():
        def turn(i, carry):
            at = pl.ds(pl.multiple_of(i * LANES, LANES), LANES)
            wt_out[at, :] = wt_t[:, at].T
            return carry

        lax.fori_loop(0, n // LANES, turn, 0)
        w[...] = w_f32[...].astype(BF16)
        fill_rows(table, halo, n, blocks)

        fill_rows(table, feats, 0, blocks)

        def pick(i, carry):
            for u in range(8):
                j = i * 8 + u
                list_wt[pl.ds(j, 1), :] = wt_out[pl.ds(lists[j], 1), :]
            return carry

        lax.fori_loop(0, rows // 8, pick, 0)
        gather_rows(rows // STEP, lambda j: lists[j], src, list_wt, table, zbuf, wbuf)
        h = hidden(aggregate())
        for c in range(h.shape[1] // LANES):
            zbuf[pl.ds(c, rows, stride=8), :] = h[:, c * LANES : (c + 1) * LANES]
        second[...] = zbuf[...].astype(BF16)

    @pl.when(g > 0)
    def _():
        first_row = pl.multiple_of((g - 1) * rows, rows)
        gather_rows(rows // STEP, lambda j: first_row + j, src, wt_out.at[pl.ds(first_row, rows)], table, zbuf, wbuf)
        z = aggregate()
        z_out[...] = z
        h_out[...] = hidden(z).astype(BF16)


def layer_two_kernel(classes, deg, inv_total, *refs):
    src, (wt, own, halo, w, label, g_out, gw_out, table, zbuf, wbuf, loss_sum) = refs[:deg], refs[deg:]
    g = pl.program_id(0)
    rows, blocks = g_out.shape[0], own.shape[1] // LANES

    @pl.when(g == 0)
    def _():
        fill_rows(table, own, 0, blocks)
        fill_tiles(table, halo, own.shape[0])
        gw_out[...] = jnp.zeros_like(gw_out)
        loss_sum[...] = jnp.zeros_like(loss_sum)

    first_row = g * rows
    gather_rows(rows // STEP, lambda j: first_row + j, src, wt, table, zbuf, wbuf)
    z = jnp.concatenate([zbuf[pl.ds(c, rows, stride=8), :] for c in range(blocks)], axis=1).astype(BF16)
    logits = jnp.dot(z, w[...], preferred_element_type=F32)
    col = lax.broadcasted_iota(jnp.int32, logits.shape, 1)
    real = col < classes
    top = jnp.max(jnp.where(real, logits, -jnp.inf), axis=1, keepdims=True)
    shifted = logits - top
    log_sum = jnp.log(jnp.sum(jnp.where(real, jnp.exp(shifted), 0.0), axis=1, keepdims=True))
    log_prob = shifted - log_sum
    tag = label[...]
    hit = col == tag
    loss_sum[...] += jnp.sum(jnp.where(hit, log_prob, 0.0), axis=0, keepdims=True)
    scale = jnp.where(tag >= 0, inv_total[0], 0.0)
    grad = jnp.where(real, (jnp.exp(log_prob) - jnp.where(hit, 1.0, 0.0)) * scale, 0.0).astype(BF16)
    g_out[...] = grad
    gw_out[...] += lax.dot_general(grad, z, (((0,), (0,)), ((), ())), preferred_element_type=F32)

    @pl.when(g == pl.num_programs(0) - 1)
    def _():
        total = jnp.sum(loss_sum[...], axis=1, keepdims=True)
        gw_out[pl.ds(gw_out.shape[0] - 1, 1), pl.ds(0, LANES)] = jnp.broadcast_to(total, (1, LANES))


def scatter_kernel(deg, *refs):
    src, (wt, grad, s_out, gbuf, wbuf), parts = refs[:deg], refs[deg : deg + 5], refs[deg + 5 :]
    g = pl.program_id(0)
    rows = grad.shape[0]
    steps = rows // STEP

    @pl.when(g == 0)
    def _():
        def clear(i, carry):
            for part in parts:
                for j in range(8):
                    part[pl.ds(pl.multiple_of(i * 64, 64) + j * 8, 8), :] = jnp.zeros((8, LANES), F32)
            return carry

        lax.fori_loop(0, s_out.shape[0] // 64, clear, 0)

    x = grad[...].astype(F32)
    for c in range(2):
        gbuf[pl.ds(c, rows, stride=2), :] = x[:, c * LANES : (c + 1) * LANES]

    def put(i):
        put_weights(wbuf, wt[pl.ds(pl.multiple_of(i * STEP, STEP), STEP), :])

    put(0)

    def step(i, carry):
        here = gbuf.at[pl.ds(pl.multiple_of(i * STEP * 2, STEP * 2), STEP * 2)]
        for u in range(STEP):
            row = here[pl.ds(u * 2, 2), :]
            n = g * rows + i * STEP + u
            for k in range(deg):
                at = pl.ds(pl.multiple_of(src[k][n], 2), 2)
                w = wbuf[pl.ds((u // 8 * deg + k) * 8 + u % 8, 2, stride=0), :]
                parts[k][at, :] = parts[k][at, :] + row * w
        put(jnp.minimum(i + 1, steps - 1))
        return carry

    lax.fori_loop(0, steps, step, 0)

    @pl.when(g == pl.num_programs(0) - 1)
    def _():
        def add(i, carry):
            at = pl.ds(pl.multiple_of(i * 64, 64), 64)
            total = parts[0][at, :]
            for part in parts[1:]:
                total = total + part[at, :]
            s_out[at, :] = total
            return carry

        lax.fori_loop(0, s_out.shape[0] // 64, add, 0)


def backward_kernel(lists, own, back, w_t, gw_two, h, z, gw_out, total):
    g = pl.program_id(0)
    rows = h.shape[0]

    @pl.when(g == 0)
    def _():
        f_in = z.shape[1]
        gw_out[pl.ds(0, f_in), :] = jnp.zeros((f_in, gw_out.shape[1]), F32)
        gw_out[pl.ds(f_in, gw_two.shape[0]), :] = gw_two[...]

        def copy(i, carry):
            at = pl.ds(pl.multiple_of(i * 64, 64), 64)
            total[at, :] = own[at, :]
            return carry

        lax.fori_loop(0, own.shape[0] // 64, copy, 0)

        def add(i, carry):
            for j in range(4):
                at = pl.ds(pl.multiple_of(lists[i * 4 + j], 2), 2)
                total[at, :] = total[at, :] + back[pl.ds(pl.multiple_of(i * 8, 8) + j * 2, 2), :]
            return carry

        lax.fori_loop(0, back.shape[0] // 8, add, 0)

    s = jnp.concatenate([total[pl.ds(g * rows * 2 + c, rows, stride=2), :] for c in range(2)], axis=1)
    high = s.astype(BF16)
    rest = s - high.astype(F32)
    mid = rest.astype(BF16)
    low = (rest - mid.astype(F32)).astype(BF16)
    wt = w_t[...]
    d = jnp.dot(low, wt, preferred_element_type=F32)
    d = d + jnp.dot(mid, wt, preferred_element_type=F32)
    d = d + jnp.dot(high, wt, preferred_element_type=F32)
    grad = jnp.where(h[...] > 0, d, 0.0).astype(BF16)
    gw_out[pl.ds(0, z.shape[1]), :] += lax.dot_general(z[...], grad, (((0,), (0,)), ((), ())), preferred_element_type=F32)


MESH = pl.DeviceIdType.MESH
SIDE = 4
COLORS = ((0, 384, (0, 1, 2)), (384, 384, (1, 2, 0)), (768, 256, (2, 0, 1)))


def reduce_kernel(x, out, acc, pair_buf, relay, far, mid, near, *sems):
    pair_send, pair_recv, ring_send, ring_recv, rs_send, rs_recv, ag_send, ag_recv, back_send, back_recv = sems
    me = lax.axis_index("graph")
    core = lax.rem(me, 2)
    where = [lax.rem(me // (2 * SIDE**d), SIDE) for d in range(3)]
    partner = me + 1 - 2 * core
    half = acc.shape[0]
    big = half // SIDE

    def peer(axis, t):
        p = lax.rem(where[axis] + t, SIDE)
        return p, me + (p - where[axis]) * (2 * SIDE**axis)

    barrier = pltpu.get_barrier_semaphore()
    pl.semaphore_signal(barrier, inc=1, device_id=(partner,), device_id_type=MESH)
    for axis in range(3):
        for t in range(1, SIDE):
            pl.semaphore_signal(barrier, inc=1, device_id=(peer(axis, t)[1],), device_id_type=MESH)
    pl.semaphore_wait(barrier, 10)
    pending = []

    def send(src, dst, send_sem, recv_sem, dev):
        copy = pltpu.make_async_remote_copy(
            src_ref=src, dst_ref=dst, send_sem=send_sem, recv_sem=recv_sem, device_id=(dev,), device_id_type=MESH
        )
        copy.start()
        pending.append(copy)
        return copy

    base, other = pl.multiple_of(core * half, 8), pl.multiple_of(half - core * half, 8)
    colors = [(pl.ds(lane, width), axes) for lane, width, axes in COLORS]

    def piece(c, t, part, start=0):
        p, _ = peer(colors[c][1][0], t)
        return pl.ds(pl.multiple_of(start + p * big + part * (big // 2), 8), big // 2)

    order = ((2, 0), (2, 1), (1, 1), (3, 0), (1, 0), (3, 1), (0, 0), (0, 1))
    pair = {}
    for t, part in order:
        for c, (lanes, _) in enumerate(colors):
            at = piece(c, t, part)
            pair[c, t, part] = send(
                x.at[piece(c, t, part, other), lanes], pair_buf.at[at, lanes], pair_send.at[c, t * 2 + part], pair_recv.at[c, t * 2 + part], partner
            )
    ring = {}
    for t, part in order:
        for c, (lanes, axes) in enumerate(colors):
            at = piece(c, t, part)
            pair[c, t, part].wait_recv()
            mine = x[piece(c, t, part, base), lanes] + pair_buf[at, lanes]
            if (t, part) in ((1, 0), (3, 1)):
                ring[c, 2, part].wait_recv()
                mine = mine + relay[part, :, lanes]
            acc[at, lanes] = mine
            if t == 0:
                continue
            forward = part == 0 if t == 2 else t == 1
            _, dev = peer(axes[0], 1 if forward else 3)
            if t == 2:
                dst = relay.at[part, :, lanes]
            else:
                dst = far.at[0 if forward else 1, pl.ds(part * (big // 2), big // 2), lanes]
            slot = order.index((t, part))
            ring[c, t, part] = send(acc.at[at, lanes], dst, ring_send.at[0, c, slot], ring_recv.at[0, c, slot], dev)
    start = [0, 0, 0]
    for c, (lanes, axes) in enumerate(colors):
        start[c] = where[axes[0]] * big
        for key in ((1, 1), (3, 0), (1, 0), (3, 1)):
            ring[(c, *key)].wait_recv()
        rows = pl.ds(pl.multiple_of(start[c], 8), big)
        acc[rows, lanes] = acc[rows, lanes] + far[0, :, lanes] + far[1, :, lanes]
    for stage, (size, buf) in enumerate(((big // SIDE, mid), (big // SIDE**2, near)), 1):
        copies = {}
        for c, (lanes, axes) in enumerate(colors):
            for t in (2, 1, 3):
                p, dev = peer(axes[stage], t)
                rows = pl.ds(pl.multiple_of(start[c] + p * size, 8), size)
                sem = (stage - 1, c, t - 1)
                copies[c, t] = send(acc.at[rows, lanes], buf.at[t - 1, :, lanes], rs_send.at[sem], rs_recv.at[sem], dev)
        for c, (lanes, axes) in enumerate(colors):
            start[c] = start[c] + where[axes[stage]] * size
            rows = pl.ds(pl.multiple_of(start[c], 8), size)
            for t in (1, 2, 3):
                copies[c, t].wait_recv()
            mine = acc[rows, lanes] + buf[0, :, lanes] + buf[1, :, lanes] + buf[2, :, lanes]
            if stage == 1:
                acc[rows, lanes] = mine
            else:
                out[pl.ds(pl.multiple_of(base + start[c], 8), size), lanes] = mine
    for stage, size in ((2, big // SIDE**2), (1, big // SIDE)):
        copies = {}
        for c, (lanes, axes) in enumerate(colors):
            here = out.at[pl.ds(pl.multiple_of(base + start[c], 8), size), lanes]
            for t in (2, 1, 3):
                _, dev = peer(axes[stage], t)
                sem = (stage - 1, c, t - 1)
                copies[c, t] = send(here, here, ag_send.at[sem], ag_recv.at[sem], dev)
        for c, (lanes, axes) in enumerate(colors):
            for t in (1, 2, 3):
                copies[c, t].wait_recv()
            start[c] = start[c] - where[axes[stage]] * size
    got = {}

    def pass_on(c, t, part, slot, directions):
        here = out.at[piece(c, t, part, base), colors[c][0]]
        for d, name in directions:
            _, dev = peer(colors[c][1][0], d)
            got[c, name] = send(here, here, ring_send.at[1, c, name], ring_recv.at[1, c, name], dev)
        got[c, slot] = send(here, here, back_send.at[c, slot - 6], back_recv.at[c, slot - 6], partner)

    for c in range(3):
        pass_on(c, 0, 0, 6, ((1, 0), (3, 3)))
        pass_on(c, 0, 1, 7, ((3, 2), (1, 1)))
    for c in range(3):
        got[c, 0].wait_recv()
        pass_on(c, 3, 0, 8, ((1, 4),))
        got[c, 2].wait_recv()
        pass_on(c, 1, 1, 9, ((3, 5),))
    for name, (t, part), slot in ((1, (3, 1), 10), (3, (1, 0), 11), (4, (2, 0), 12), (5, (2, 1), 13)):
        for c in range(3):
            got[c, name].wait_recv()
            pass_on(c, t, part, slot, ())
    for c in range(3):
        for slot in range(6, 14):
            got[c, slot].wait_recv()
    for copy in pending:
        copy.wait_send()


def reduce_all(x):
    sem = pltpu.SemaphoreType.DMA
    return pl.pallas_call(reduce_kernel,
        in_specs=[pl.BlockSpec(memory_space=pltpu.VMEM)], out_specs=pl.BlockSpec(memory_space=pltpu.VMEM),
        out_shape=jax.ShapeDtypeStruct((1024,1024),F32),
        scratch_shapes=[pltpu.VMEM((512,1024),F32), pltpu.VMEM((512,1024),F32), pltpu.VMEM((2,64,1024),F32), pltpu.VMEM((2,128,1024),F32), pltpu.VMEM((3,32,1024),F32), pltpu.VMEM((3,8,1024),F32),
            sem((3,8)), sem((3,8)), sem((2,3,6)), sem((2,3,6)), sem((2,3,3)), sem((2,3,3)), sem((2,3,3)), sem((2,3,3)), sem((3,8)), sem((3,8))],
        compiler_params=pltpu.CompilerParams(collective_id=0, has_side_effects=True, vmem_limit_bytes=40*2**20),
        name="reduce_all")(x)


def count_kernel(x, out, came, send, recv):
    me = lax.axis_index("graph")
    hops = [(1, 2)] + [(2 * SIDE**axis, SIDE) for axis in range(3)]

    def peer(stride, size, t):
        here = lax.rem(me // stride, size)
        return me + (lax.rem(here + t, size) - here) * stride

    barrier = pltpu.get_barrier_semaphore()
    for stride, size in hops:
        for t in range(1, size):
            pl.semaphore_signal(barrier, inc=1, device_id=(peer(stride, size, t),), device_id_type=MESH)
    pl.semaphore_wait(barrier, came.shape[0])
    out[0] = x[...]
    slot = 0
    copies = []
    for stage, (stride, size) in enumerate(hops):
        step = []
        for t in range(1, size):
            at = slot + t - 1
            step.append(
                pltpu.make_async_remote_copy(
                    src_ref=out.at[stage],
                    dst_ref=came.at[at],
                    send_sem=send.at[at],
                    recv_sem=recv.at[at],
                    device_id=(peer(stride, size, t),),
                    device_id_type=MESH,
                )
            )
            step[-1].start()
        total = out[stage]
        for t, copy in enumerate(step):
            copy.wait_recv()
            total = total + came[slot + t]
        out[stage + 1] = total
        slot += size - 1
        copies += step
    for copy in copies:
        copy.wait_send()


def count_all(x):
    vmem = pl.BlockSpec(memory_space=pltpu.VMEM)
    return pl.pallas_call(
        count_kernel,
        in_specs=[vmem],
        out_specs=vmem,
        out_shape=jax.ShapeDtypeStruct((5, 8, LANES), F32),
        scratch_shapes=[pltpu.VMEM((10, 8, LANES), F32), pltpu.SemaphoreType.DMA((10,)), pltpu.SemaphoreType.DMA((10,))],
        compiler_params=pltpu.CompilerParams(collective_id=1, has_side_effects=True, vmem_limit_bytes=2**20),
        name="count_all",
    )(x)


def params():
    return pltpu.CompilerParams(dimension_semantics=("arbitrary",), vmem_limit_bytes=62 * 2**20)


SMEM = pl.BlockSpec(memory_space=pltpu.SMEM)


def solution(mesh):
    dev_count = mesh.shape["graph"]

    def device_step(feats, w_one, w_two, send_idx, send_count, edge_src, edge_wt, labels, label_mask):
        n, f_in = feats.shape
        f_hid, classes = w_two.shape
        halo_rows, deg = send_idx.shape[1], edge_src.shape[1]
        halo = dev_count * halo_rows
        ext = n + halo
        pad = 2 * LANES
        w_two_b = jnp.pad(w_two.astype(BF16), ((0, 0), (0, pad - classes)))
        list_ids = send_idx.reshape(halo)
        lists2 = list_ids * 2
        src8 = [edge_src[:, k] * 8 for k in range(deg)]
        src2 = [edge_src[:, k] * 2 for k in range(deg)]
        count = jnp.sum(label_mask.astype(F32))
        first_rows, count = lax.optimization_barrier((feats[list_ids], count))
        first_in = lax.all_to_all(first_rows, "graph", 0, 0, tiled=True)
        label_total = count_all(jnp.full((8, LANES), count))[4, 0, 0]
        first_in, label_total = lax.optimization_barrier((first_in, label_total))
        inv_total = (1.0 / label_total).reshape(1)
        label = jnp.where(label_mask == 1, labels, -1).reshape(n, 1)

        def by_rows(width):
            return pl.BlockSpec((BLOCK, width), lambda g: (g, 0))

        def after_first(width):
            return pl.BlockSpec((BLOCK, width), lambda g: (jnp.maximum(g - 1, 0), 0))

        gather_scratch = [
            pltpu.VMEM((ext * 8, LANES), F32),
            pltpu.VMEM((BLOCK * 8, LANES), F32),
            pltpu.VMEM((STEP * deg + 8, LANES), F32),
        ]
        z_one, h_one, wt, second = pl.pallas_call(
            functools.partial(layer_one_kernel, deg),
            grid=(1 + n // BLOCK,),
            in_specs=[SMEM] + [SMEM] * deg + [once((n, f_in)), once((halo, f_in)), once((deg, n)), once((f_in, f_hid))],
            out_specs=[after_first(f_in), after_first(f_hid), once((n, deg)), once((halo * 8, LANES))],
            out_shape=[
                jax.ShapeDtypeStruct((n, f_in), BF16),
                jax.ShapeDtypeStruct((n, f_hid), BF16),
                jax.ShapeDtypeStruct((n, deg), F32),
                jax.ShapeDtypeStruct((halo * 8, LANES), BF16),
            ],
            scratch_shapes=gather_scratch
            + [
                pltpu.VMEM((f_in, f_hid), BF16),
                pltpu.VMEM((halo, deg), F32),
            ],
            compiler_params=params(),
            name="layer_one",
        )(list_ids, *src8, feats, first_in, edge_wt.T, w_one)
        h_in = lax.all_to_all(second, "graph", 0, 0, tiled=True)
        grad_log, gw_two = pl.pallas_call(
            functools.partial(layer_two_kernel, classes, deg),
            grid=(n // BLOCK,),
            in_specs=[SMEM] + [SMEM] * deg + [by_rows(deg), once((n, f_hid)), once((halo * 8, LANES)), once((f_hid, pad)), by_rows(1)],
            out_specs=[by_rows(pad), once((pad, f_hid))],
            out_shape=[jax.ShapeDtypeStruct((n, pad), BF16), jax.ShapeDtypeStruct((pad, f_hid), F32)],
            scratch_shapes=gather_scratch + [pltpu.VMEM((1, pad), F32)],
            compiler_params=params(),
            name="layer_two",
        )(inv_total, *src8, wt, h_one, h_in, w_two_b, label)
        ext_grad = pl.pallas_call(
            functools.partial(scatter_kernel, deg),
            grid=(n // 512,),
            in_specs=[SMEM] * deg + [by_rows(deg), by_rows(pad)],
            out_specs=once((ext * 2, LANES)),
            out_shape=jax.ShapeDtypeStruct((ext * 2, LANES), F32),
            scratch_shapes=[pltpu.VMEM((BLOCK * 2, LANES), F32), pltpu.VMEM((STEP * deg + 8, LANES), F32)]
            + [pltpu.VMEM((ext * 2, LANES), F32) for _ in range(deg)],
            compiler_params=params(),
            name="scatter",
        )(*src2, wt, grad_log)
        back = lax.all_to_all(ext_grad[n * 2 :], "graph", 0, 0, tiled=True)
        partial = pl.pallas_call(
            backward_kernel,
            grid=(n // 512,),
            in_specs=[
                SMEM,
                once((n * 2, LANES)),
                once((halo * 2, LANES)),
                once((pad, f_hid)),
                once((pad, f_hid)),
                pl.BlockSpec((512, f_hid), lambda g: (g, 0)),
                pl.BlockSpec((512, f_in), lambda g: (g, 0)),
            ],
            out_specs=once((f_in + pad, f_hid)),
            out_shape=jax.ShapeDtypeStruct((f_in + pad, f_hid), F32),
            scratch_shapes=[pltpu.VMEM((n * 2 + 8, LANES), F32)],
            compiler_params=params(),
            name="backward",
        )(lists2, ext_grad, back, w_two_b.T, gw_two, h_one, z_one)
        total = reduce_all(partial)
        return -total[f_in + pad - 1, 0] / label_total, total[:f_in], total[f_in : f_in + classes].T

    row_spec = P("graph", None)
    vec_spec = P("graph")
    return jax.shard_map(
        device_step,
        mesh=mesh,
        in_specs=(row_spec, P(), P(), row_spec, vec_spec, row_spec, row_spec, vec_spec, vec_spec),
        out_specs=(P(), P(), P()),
        check_vma=False,
    )
```

```python
import functools

import jax
import jax.numpy as jnp
from jax import lax
from jax.experimental import pallas as pl
from jax.experimental.pallas import tpu as pltpu
from jax.sharding import PartitionSpec as P

LANES = 128
TAIL = 32
STEP = 16
BLOCK = 512
F32, BF16 = jnp.float32, jnp.bfloat16


def once(shape):
    return pl.BlockSpec(shape, lambda g: (0,) * len(shape), pipeline_mode=pl.Buffered(1))


def fill_rows(dst, src, offset, blocks):
    def step(i, carry):
        r = pl.multiple_of(i * 64, 64)
        x = src[pl.ds(r, 64), :].astype(F32)
        for c in range(blocks):
            dst[pl.ds((r + offset) * 8 + c, 64, stride=8), :] = x[:, c * LANES : (c + 1) * LANES]
        return carry

    lax.fori_loop(0, src.shape[0] // 64, step, 0)


def put_weights(wbuf, w):
    deg = w.shape[1]
    for h in range(STEP // 8):
        for k in range(deg):
            tile = jnp.broadcast_to(w[h * 8 : h * 8 + 8, k : k + 1], (8, LANES))
            wbuf[pl.ds((h * deg + k) * 8, 8), :] = tile


def gather_rows(steps, row_of, src, wt, table, out, wbuf):
    deg = wt.shape[1]

    def put(i):
        put_weights(wbuf, wt[pl.ds(pl.multiple_of(i * STEP, STEP), STEP), :])

    put(0)

    def step(i, carry):
        dst = out.at[pl.ds(pl.multiple_of(i * STEP * 8, STEP * 8), STEP * 8)]
        for u in range(STEP):
            n = row_of(i * STEP + u)
            acc = None
            for k in range(deg):
                row = table[pl.ds(pl.multiple_of(src[k][n], 8), 8), :]
                term = row * wbuf[pl.ds((u // 8 * deg + k) * 8 + u % 8, 8, stride=0), :]
                acc = term if acc is None else acc + term
            dst[pl.ds(u * 8, 8), :] = acc
        put(jnp.minimum(i + 1, steps - 1))
        return carry

    lax.fori_loop(0, steps, step, 0)


def load_sources(src_hbm, src, sems):
    copies = [pltpu.make_async_copy(hbm, ref, sems.at[k]) for k, (hbm, ref) in enumerate(zip(src_hbm, src))]
    for copy in copies:
        copy.start()
    return copies


def fill_tiles(dst, src, offset):
    def step(i, carry):
        at = pl.multiple_of(i * 128, 128)
        dst[pl.ds(pl.multiple_of(offset * 8 + at, 8), 128), :] = src[pl.ds(at, 128), :].astype(F32)
        return carry

    lax.fori_loop(0, src.shape[0] // 128, step, 0)


def fill_from(table, hbm, chunk, sems, blocks):
    rows = chunk.shape[1]
    steps = hbm.shape[0] // rows

    def fetch(i):
        slot = lax.rem(i, 2)
        return pltpu.make_async_copy(hbm.at[pl.ds(pl.multiple_of(i * rows, rows), rows), :], chunk.at[slot], sems.at[slot])

    fetch(0).start()

    def take(i, carry):
        @pl.when(i + 1 < steps)
        def _():
            fetch(i + 1).start()

        fetch(i).wait()
        slot = lax.rem(i, 2)

        def fill(j, carry):
            r = pl.multiple_of(j * 64, 64)
            x = chunk[slot, pl.ds(r, 64), :].astype(F32)
            for c in range(blocks):
                table[pl.ds((i * rows + r) * 8 + c, 64, stride=8), :] = x[:, c * LANES : (c + 1) * LANES]
            return carry

        return lax.fori_loop(0, rows // 64, fill, carry)

    lax.fori_loop(0, steps, take, 0)


def first_layer(zbuf, w, rows, blocks):
    z = jnp.concatenate([zbuf[pl.ds(c, rows, stride=8), :] for c in range(blocks)], axis=1).astype(BF16)
    return z, jnp.maximum(jnp.dot(z, w[...], preferred_element_type=F32), 0.0)


def list_rows_kernel(deg, lists, *refs):
    src_hbm, refs, src = refs[:deg], refs[deg:-deg], refs[-deg:]
    feats, halo, wt, w, second, table, zbuf, wbuf, list_wt, chunk, src_sem, chunk_sem = refs
    rows, blocks = list_wt.shape[0], feats.shape[1] // LANES
    index_copies = load_sources(src_hbm, src, src_sem)
    fill_rows(table, halo, feats.shape[0], blocks)
    fill_from(table, feats, chunk, chunk_sem, blocks)

    def pick(i, carry):
        for u in range(8):
            j = i * 8 + u
            list_wt[pl.ds(j, 1), :] = wt[pl.ds(lists[j], 1), :]
        return carry

    lax.fori_loop(0, rows // 8, pick, 0)
    for copy in index_copies:
        copy.wait()
    gather_rows(rows // STEP, lambda j: lists[j], src, list_wt, table, zbuf, wbuf)
    _, h = first_layer(zbuf, w, rows, blocks)
    for c in range(h.shape[1] // LANES):
        zbuf[pl.ds(c, rows, stride=8), :] = h[:, c * LANES : (c + 1) * LANES]
    second[...] = zbuf[...].astype(BF16)


def layer_one_kernel(deg, *refs):
    src_hbm, refs, src = refs[:deg], refs[deg:-deg], refs[-deg:]
    feats, halo, wt, w, z_out, h_out, table, zbuf, wbuf, chunk, src_sem, chunk_sem = refs
    g = pl.program_id(0)
    rows, blocks = z_out.shape[0], feats.shape[1] // LANES

    @pl.when(g == 0)
    def _():
        index_copies = load_sources(src_hbm, src, src_sem)
        fill_rows(table, halo, feats.shape[0], blocks)
        fill_from(table, feats, chunk, chunk_sem, blocks)
        for copy in index_copies:
            copy.wait()

    first_row = pl.multiple_of(g * rows, rows)
    gather_rows(rows // STEP, lambda j: first_row + j, src, wt, table, zbuf, wbuf)
    z, h = first_layer(zbuf, w, rows, blocks)
    z_out[...] = z
    h_out[...] = h.astype(BF16)


def layer_two_kernel(classes, deg, inv_total, *refs):
    src_hbm, refs, src = refs[:deg], refs[deg:-deg], refs[-deg:]
    wt, own, halo, w, label, g_out, z_out, loss_out, table, zbuf, wbuf, loss_sum, chunk, src_sem, chunk_sem = refs
    g = pl.program_id(0)
    rows, blocks = g_out.shape[0], own.shape[1] // LANES

    @pl.when(g == 0)
    def _():
        index_copies = load_sources(src_hbm, src, src_sem)
        loss_sum[...] = jnp.zeros_like(loss_sum)
        fill_tiles(table, halo, own.shape[0])
        fill_from(table, own, chunk, chunk_sem, blocks)
        for copy in index_copies:
            copy.wait()

    first_row = g * rows
    gather_rows(rows // STEP, lambda j: first_row + j, src, wt, table, zbuf, wbuf)
    z = jnp.concatenate([zbuf[pl.ds(c, rows, stride=8), :] for c in range(blocks)], axis=1).astype(BF16)
    logits = jnp.dot(z, w[...], preferred_element_type=F32)
    col = lax.broadcasted_iota(jnp.int32, logits.shape, 1)
    real = col < classes
    top = jnp.max(jnp.where(real, logits, -jnp.inf), axis=1, keepdims=True)
    shifted = logits - top
    log_sum = jnp.log(jnp.sum(jnp.where(real, jnp.exp(shifted), 0.0), axis=1, keepdims=True))
    log_prob = shifted - log_sum
    tag = label[...]
    hit = col == tag
    loss_sum[...] += jnp.sum(jnp.where(hit, log_prob, 0.0), axis=0, keepdims=True)
    scale = jnp.where(tag >= 0, inv_total[0], 0.0)
    grad = jnp.where(real, (jnp.exp(log_prob) - jnp.where(hit, 1.0, 0.0)) * scale, 0.0).astype(BF16)
    g_out[...] = grad
    z_out[...] = z

    @pl.when(g == pl.num_programs(0) - 1)
    def _():
        loss_out[...] = jnp.broadcast_to(jnp.sum(loss_sum[...], axis=1, keepdims=True), loss_out.shape)


def grad_two_kernel(grad, z, loss, gw_out):
    g = pl.program_id(0)

    @pl.when(g == 0)
    def _():
        gw_out[...] = jnp.zeros_like(gw_out)

    gw_out[...] += lax.dot_general(grad[...], z[...], (((0,), (0,)), ((), ())), preferred_element_type=F32)

    @pl.when(g == pl.num_programs(0) - 1)
    def _():
        gw_out[pl.ds(gw_out.shape[0] - 1, 1), pl.ds(0, LANES)] = loss[...]


def scatter_kernel(deg, *refs):
    src_hbm, (wt, grad, s_out, gbuf, wbuf, sems), refs = refs[:deg], refs[deg : deg + 6], refs[deg + 6 :]
    src, parts = refs[:deg], refs[deg:]
    g = pl.program_id(0)
    rows = grad.shape[0]
    steps = rows // STEP

    @pl.when(g == 0)
    def _():
        index_copies = load_sources(src_hbm, src, sems)

        def clear(i, carry):
            for part in parts:
                for j in range(8):
                    part[pl.ds(pl.multiple_of(i * 64, 64) + j * 8, 8), :] = jnp.zeros((8, LANES), F32)
            return carry

        lax.fori_loop(0, s_out.shape[0] // 64, clear, 0)
        for copy in index_copies:
            copy.wait()

    x = grad[...].astype(F32)
    for c in range(2):
        gbuf[pl.ds(c, rows, stride=2), :] = x[:, c * LANES : (c + 1) * LANES]

    def put(i):
        put_weights(wbuf, wt[pl.ds(pl.multiple_of(i * STEP, STEP), STEP), :])

    put(0)

    def step(i, carry):
        here = gbuf.at[pl.ds(pl.multiple_of(i * STEP * 2, STEP * 2), STEP * 2)]
        for u in range(STEP):
            row = here[pl.ds(u * 2, 2), :]
            n = g * rows + i * STEP + u
            for k in range(deg):
                at = pl.ds(pl.multiple_of(src[k][n], 2), 2)
                w = wbuf[pl.ds((u // 8 * deg + k) * 8 + u % 8, 2, stride=0), :]
                parts[k][at, :] = parts[k][at, :] + row * w
        put(jnp.minimum(i + 1, steps - 1))
        return carry

    lax.fori_loop(0, steps, step, 0)

    @pl.when(g == pl.num_programs(0) - 1)
    def _():
        def add(i, carry):
            at = pl.ds(pl.multiple_of(i * 64, 64), 64)
            total = parts[0][at, :]
            for part in parts[1:]:
                total = total + part[at, :]
            s_out[at, :] = total
            return carry

        lax.fori_loop(0, s_out.shape[0] // 64, add, 0)


def backward_kernel(lists, own, back, w_t, gw_two, h_hbm, z_hbm, gw_out, total, h, z, own_sem, sems):
    n, f_in = z.shape
    rows = BLOCK
    own_copy = pltpu.make_async_copy(own.at[pl.ds(0, total.shape[0])], total, own_sem)
    own_copy.start()

    def fetch(i):
        at = pl.ds(pl.multiple_of(i * rows, rows), rows)
        return (
            pltpu.make_async_copy(h_hbm.at[at], h.at[at], sems.at[0, i]),
            pltpu.make_async_copy(z_hbm.at[at], z.at[at], sems.at[1, i]),
        )

    def begin(i, carry):
        for copy in fetch(i):
            copy.start()
        return carry

    lax.fori_loop(0, n // rows, begin, 0)
    gw_out[pl.ds(0, f_in), :] = jnp.zeros((f_in, gw_out.shape[1]), F32)
    gw_out[pl.ds(f_in, gw_two.shape[0]), :] = gw_two[...]

    own_copy.wait()

    def add(i, carry):
        for j in range(4):
            at = pl.ds(pl.multiple_of(lists[i * 4 + j], 2), 2)
            total[at, :] = total[at, :] + back[pl.ds(pl.multiple_of(i * 8, 8) + j * 2, 2), :]
        return carry

    lax.fori_loop(0, back.shape[0] // 8, add, 0)

    def block(i, carry):
        for copy in fetch(i):
            copy.wait()
        at = pl.ds(pl.multiple_of(i * rows, rows), rows)
        parts = []
        for c in range(2):
            s = total[pl.ds(i * rows * 2 + c, rows, stride=2), :]
            high = s.astype(BF16).astype(F32)
            mid = (s - high).astype(BF16).astype(F32)
            parts.append((high, mid, s - high - mid))
        tail = parts[1][0] + pltpu.roll(parts[1][1], TAIL, 1) + pltpu.roll(parts[1][2], 2 * TAIL, 1)
        d = jnp.dot(jnp.concatenate([*parts[0], tail], axis=1).astype(BF16), w_t[...], preferred_element_type=F32)
        grad = jnp.where(h[at, :] > 0, d, 0.0).astype(BF16)
        gw_out[pl.ds(0, f_in), :] += lax.dot_general(z[at, :], grad, (((0,), (0,)), ((), ())), preferred_element_type=F32)
        return carry

    lax.fori_loop(0, n // rows, block, 0)


MESH = pl.DeviceIdType.MESH
SIDE = 4
COLORS = ((0, 384, (0, 1, 2)), (384, 384, (1, 2, 0)), (768, 256, (2, 0, 1)))


def reduce_kernel(x, out, acc, pair_buf, relay, far, mid, near, *sems):
    pair_send, pair_recv, ring_send, ring_recv, rs_send, rs_recv, ag_send, ag_recv, back_send, back_recv = sems
    me = lax.axis_index("graph")
    core = lax.rem(me, 2)
    where = [lax.rem(me // (2 * SIDE**d), SIDE) for d in range(3)]
    partner = me + 1 - 2 * core
    half = acc.shape[0]
    big = half // SIDE

    def peer(axis, t):
        p = lax.rem(where[axis] + t, SIDE)
        return p, me + (p - where[axis]) * (2 * SIDE**axis)

    barrier = pltpu.get_barrier_semaphore()
    pl.semaphore_signal(barrier, inc=1, device_id=(partner,), device_id_type=MESH)
    for axis in range(3):
        for t in range(1, SIDE):
            pl.semaphore_signal(barrier, inc=1, device_id=(peer(axis, t)[1],), device_id_type=MESH)
    pl.semaphore_wait(barrier, 10)
    pending = []

    def send(src, dst, send_sem, recv_sem, dev):
        copy = pltpu.make_async_remote_copy(
            src_ref=src, dst_ref=dst, send_sem=send_sem, recv_sem=recv_sem, device_id=(dev,), device_id_type=MESH
        )
        copy.start()
        pending.append(copy)
        return copy

    base, other = pl.multiple_of(core * half, 8), pl.multiple_of(half - core * half, 8)
    colors = [(pl.ds(lane, width), axes) for lane, width, axes in COLORS]

    def piece(c, t, part, start=0):
        p, _ = peer(colors[c][1][0], t)
        return pl.ds(pl.multiple_of(start + p * big + part * (big // 2), 8), big // 2)

    order = ((2, 0), (2, 1), (1, 1), (3, 0), (1, 0), (3, 1), (0, 0), (0, 1))
    pair = {}
    for t, part in order:
        for c, (lanes, _) in enumerate(colors):
            at = piece(c, t, part)
            pair[c, t, part] = send(
                x.at[piece(c, t, part, other), lanes], pair_buf.at[at, lanes], pair_send.at[c, t * 2 + part], pair_recv.at[c, t * 2 + part], partner
            )
    ring = {}
    for t, part in order:
        for c, (lanes, axes) in enumerate(colors):
            at = piece(c, t, part)
            pair[c, t, part].wait_recv()
            mine = x[piece(c, t, part, base), lanes] + pair_buf[at, lanes]
            if (t, part) in ((1, 0), (3, 1)):
                ring[c, 2, part].wait_recv()
                mine = mine + relay[part, :, lanes]
            acc[at, lanes] = mine
            if t == 0:
                continue
            forward = part == 0 if t == 2 else t == 1
            _, dev = peer(axes[0], 1 if forward else 3)
            if t == 2:
                dst = relay.at[part, :, lanes]
            else:
                dst = far.at[0 if forward else 1, pl.ds(part * (big // 2), big // 2), lanes]
            slot = order.index((t, part))
            ring[c, t, part] = send(acc.at[at, lanes], dst, ring_send.at[0, c, slot], ring_recv.at[0, c, slot], dev)
    start = [0, 0, 0]
    for c, (lanes, axes) in enumerate(colors):
        start[c] = where[axes[0]] * big
        for key in ((1, 1), (3, 0), (1, 0), (3, 1)):
            ring[(c, *key)].wait_recv()
        rows = pl.ds(pl.multiple_of(start[c], 8), big)
        acc[rows, lanes] = acc[rows, lanes] + far[0, :, lanes] + far[1, :, lanes]
    for stage, (size, buf) in enumerate(((big // SIDE, mid), (big // SIDE**2, near)), 1):
        copies = {}
        for c, (lanes, axes) in enumerate(colors):
            for t in (2, 1, 3):
                p, dev = peer(axes[stage], t)
                rows = pl.ds(pl.multiple_of(start[c] + p * size, 8), size)
                sem = (stage - 1, c, t - 1)
                copies[c, t] = send(acc.at[rows, lanes], buf.at[t - 1, :, lanes], rs_send.at[sem], rs_recv.at[sem], dev)
        for c, (lanes, axes) in enumerate(colors):
            start[c] = start[c] + where[axes[stage]] * size
            rows = pl.ds(pl.multiple_of(start[c], 8), size)
            for t in (1, 2, 3):
                copies[c, t].wait_recv()
            mine = acc[rows, lanes] + buf[0, :, lanes] + buf[1, :, lanes] + buf[2, :, lanes]
            if stage == 1:
                acc[rows, lanes] = mine
            else:
                out[pl.ds(pl.multiple_of(base + start[c], 8), size), lanes] = mine
    for stage, size in ((2, big // SIDE**2), (1, big // SIDE)):
        copies = {}
        for c, (lanes, axes) in enumerate(colors):
            here = out.at[pl.ds(pl.multiple_of(base + start[c], 8), size), lanes]
            for t in (2, 1, 3):
                _, dev = peer(axes[stage], t)
                sem = (stage - 1, c, t - 1)
                copies[c, t] = send(here, here, ag_send.at[sem], ag_recv.at[sem], dev)
        for c, (lanes, axes) in enumerate(colors):
            for t in (1, 2, 3):
                copies[c, t].wait_recv()
            start[c] = start[c] - where[axes[stage]] * size
    got = {}

    def pass_on(c, t, part, slot, directions):
        here = out.at[piece(c, t, part, base), colors[c][0]]
        for d, name in directions:
            _, dev = peer(colors[c][1][0], d)
            got[c, name] = send(here, here, ring_send.at[1, c, name], ring_recv.at[1, c, name], dev)
        got[c, slot] = send(here, here, back_send.at[c, slot - 6], back_recv.at[c, slot - 6], partner)

    for c in range(3):
        pass_on(c, 0, 0, 6, ((1, 0), (3, 3)))
        pass_on(c, 0, 1, 7, ((3, 2), (1, 1)))
    for c in range(3):
        got[c, 0].wait_recv()
        pass_on(c, 3, 0, 8, ((1, 4),))
        got[c, 2].wait_recv()
        pass_on(c, 1, 1, 9, ((3, 5),))
    for name, (t, part), slot in ((1, (3, 1), 10), (3, (1, 0), 11), (4, (2, 0), 12), (5, (2, 1), 13)):
        for c in range(3):
            got[c, name].wait_recv()
            pass_on(c, t, part, slot, ())
    for c in range(3):
        for slot in range(6, 14):
            got[c, slot].wait_recv()
    for copy in pending:
        copy.wait_send()


def reduce_all(x):
    sem = pltpu.SemaphoreType.DMA
    return pl.pallas_call(reduce_kernel,
        in_specs=[pl.BlockSpec(memory_space=pltpu.VMEM)], out_specs=pl.BlockSpec(memory_space=pltpu.VMEM),
        out_shape=jax.ShapeDtypeStruct((1024,1024),F32),
        scratch_shapes=[pltpu.VMEM((512,1024),F32), pltpu.VMEM((512,1024),F32), pltpu.VMEM((2,64,1024),F32), pltpu.VMEM((2,128,1024),F32), pltpu.VMEM((3,32,1024),F32), pltpu.VMEM((3,8,1024),F32),
            sem((3,8)), sem((3,8)), sem((2,3,6)), sem((2,3,6)), sem((2,3,3)), sem((2,3,3)), sem((2,3,3)), sem((2,3,3)), sem((3,8)), sem((3,8))],
        compiler_params=pltpu.CompilerParams(collective_id=0, has_side_effects=True, vmem_limit_bytes=12*2**20),
        name="reduce_all")(x)


def exchange_kernel(n_dev, *refs):
    k = (len(refs) - 1) // 2
    sems = refs[-1]
    me = lax.axis_index("graph")

    def send(t, carry):
        q = lax.rem(me + t, n_dev)
        for j in range(k):
            src, dst = refs[j], refs[k + j]
            pltpu.make_async_remote_copy(
                src_ref=src.at[q if src.shape[0] == n_dev else 0],
                dst_ref=dst.at[me],
                send_sem=sems.at[2 * j],
                recv_sem=sems.at[2 * j + 1],
                device_id=(q,),
                device_id_type=MESH,
            ).start()
        return carry

    lax.fori_loop(1, n_dev, send, 0)
    for j in range(k):
        others = refs[k + j].at[pl.ds(0, n_dev - 1)]
        for side in range(2):
            pltpu.make_async_copy(others, others, sems.at[2 * j + side]).wait()


def exchange(n_dev, *arrays):
    vmem = pl.BlockSpec(memory_space=pltpu.VMEM)
    return pl.pallas_call(
        functools.partial(exchange_kernel, n_dev),
        in_specs=[vmem] * len(arrays),
        out_specs=[vmem] * len(arrays),
        out_shape=[jax.ShapeDtypeStruct((n_dev,) + a.shape[1:], a.dtype) for a in arrays],
        scratch_shapes=[pltpu.SemaphoreType.DMA((2 * len(arrays),))],
        compiler_params=pltpu.CompilerParams(has_side_effects=True, vmem_limit_bytes=8 * 2**20),
        name="exchange_one",
    )(*arrays)


def params():
    return pltpu.CompilerParams(dimension_semantics=("arbitrary",), vmem_limit_bytes=62 * 2**20)


SMEM = pl.BlockSpec(memory_space=pltpu.SMEM)


def solution(mesh):
    dev_count = mesh.shape["graph"]

    def device_step(feats, w_one, w_two, send_idx, send_count, edge_src, edge_wt, labels, label_mask):
        n, f_in = feats.shape
        f_hid, classes = w_two.shape
        halo_rows, deg = send_idx.shape[1], edge_src.shape[1]
        halo = dev_count * halo_rows
        ext = n + halo
        pad = 2 * LANES
        w_two_b = jnp.pad(w_two.astype(BF16), ((0, 0), (0, pad - classes)))
        list_ids = send_idx.reshape(halo)
        lists2 = list_ids * 2
        src8 = [edge_src[:, k] * 8 for k in range(deg)]
        src2 = [edge_src[:, k] * 2 for k in range(deg)]
        count = jnp.sum(label_mask.astype(F32))
        label = jnp.where(label_mask == 1, labels, -1).reshape(n, 1)
        first_in, counts = exchange(dev_count, feats[list_ids].reshape(dev_count, halo_rows, f_in), jnp.full((1, 1, LANES), count))
        first_in = first_in.reshape(halo, f_in)
        mine = jnp.arange(dev_count) == lax.axis_index("graph")
        label_total = jnp.sum(jnp.where(mine, count, counts[:, 0, 0]))
        inv_total = (1.0 / label_total).reshape(1)
        wt, w_one_b = edge_wt, w_one.astype(BF16)

        def by_rows(width):
            return pl.BlockSpec((BLOCK, width), lambda g: (g, 0))

        gather_scratch = [
            pltpu.VMEM((ext * 8, LANES), F32),
            pltpu.VMEM((BLOCK * 8, LANES), F32),
            pltpu.VMEM((STEP * deg + 8, LANES), F32),
        ]
        whole = pl.BlockSpec(memory_space=pl.ANY)
        dma = pltpu.SemaphoreType.DMA
        index_scratch = [pltpu.SMEM((n,), jnp.int32) for _ in range(deg)]

        def chunk_scratch(width):
            return [pltpu.VMEM((2, BLOCK, width), BF16), dma((deg,)), dma((2,))]

        second = pl.pallas_call(
            functools.partial(list_rows_kernel, deg),
            grid=(1,),
            in_specs=[SMEM] + [whole] * (deg + 1) + [once((halo, f_in)), once((n, deg)), once((f_in, f_hid))],
            out_specs=once((halo * 8, LANES)),
            out_shape=jax.ShapeDtypeStruct((halo * 8, LANES), BF16),
            scratch_shapes=gather_scratch + [pltpu.VMEM((halo, deg), F32)] + chunk_scratch(f_in) + index_scratch,
            compiler_params=params(),
            cost_estimate=pl.CostEstimate(flops=4 * halo * f_in * f_hid, bytes_accessed=2 * n * f_in, transcendentals=0),
            name="list_rows",
        )(list_ids, *src8, feats, first_in, wt, w_one_b)
        h_in = lax.all_to_all(second, "graph", 0, 0, tiled=True)
        z_one, h_one = pl.pallas_call(
            functools.partial(layer_one_kernel, deg),
            grid=(n // BLOCK,),
            in_specs=[whole] * (deg + 1) + [once((halo, f_in)), by_rows(deg), once((f_in, f_hid))],
            out_specs=[by_rows(f_in), by_rows(f_hid)],
            out_shape=[jax.ShapeDtypeStruct((n, f_in), BF16), jax.ShapeDtypeStruct((n, f_hid), BF16)],
            scratch_shapes=gather_scratch + chunk_scratch(f_in) + index_scratch,
            compiler_params=params(),
            cost_estimate=pl.CostEstimate(flops=8 * n * f_in * f_hid, bytes_accessed=8 * n * f_in, transcendentals=0),
            name="layer_one",
        )(*src8, feats, first_in, wt, w_one_b)
        grad_log, z_two, loss_part = pl.pallas_call(
            functools.partial(layer_two_kernel, classes, deg),
            grid=(n // BLOCK,),
            in_specs=[SMEM] + [whole] * deg + [by_rows(deg), whole, once((halo * 8, LANES)), once((f_hid, pad)), by_rows(1)],
            out_specs=[by_rows(pad), by_rows(f_hid), once((1, LANES))],
            out_shape=[
                jax.ShapeDtypeStruct((n, pad), BF16),
                jax.ShapeDtypeStruct((n, f_hid), BF16),
                jax.ShapeDtypeStruct((1, LANES), F32),
            ],
            scratch_shapes=gather_scratch + [pltpu.VMEM((1, pad), F32)] + chunk_scratch(f_hid) + index_scratch,
            compiler_params=params(),
            name="layer_two",
        )(inv_total, *src8, wt, h_one, h_in, w_two_b, label)
        ext_grad = pl.pallas_call(
            functools.partial(scatter_kernel, deg),
            grid=(n // 512,),
            in_specs=[whole] * deg + [by_rows(deg), by_rows(pad)],
            out_specs=once((ext * 2, LANES)),
            out_shape=jax.ShapeDtypeStruct((ext * 2, LANES), F32),
            scratch_shapes=[pltpu.VMEM((BLOCK * 2, LANES), F32), pltpu.VMEM((STEP * deg + 8, LANES), F32), dma((deg,))]
            + index_scratch
            + [pltpu.VMEM((ext * 2, LANES), F32) for _ in range(deg)],
            compiler_params=params(),
            name="scatter",
        )(*src2, wt, grad_log)
        returned, grad_log = lax.optimization_barrier((ext_grad[n * 2 :], grad_log))
        back = lax.all_to_all(returned, "graph", 0, 0, tiled=True)
        gw_two = pl.pallas_call(
            grad_two_kernel,
            grid=(n // BLOCK,),
            in_specs=[by_rows(pad), by_rows(f_hid), once((1, LANES))],
            out_specs=once((pad, f_hid)),
            out_shape=jax.ShapeDtypeStruct((pad, f_hid), F32),
            compiler_params=pltpu.CompilerParams(dimension_semantics=("arbitrary",), vmem_limit_bytes=20 * 2**20),
            cost_estimate=pl.CostEstimate(flops=2 * n * pad * f_hid, bytes_accessed=2 * n * f_hid, transcendentals=0),
            name="grad_two",
        )(grad_log, z_two, loss_part)
        w_t = w_two.astype(BF16).T
        w_tail = jnp.pad(w_t[LANES:], ((0, TAIL - (classes - LANES)), (0, 0)))
        w_parts = jnp.concatenate([w_t[:LANES]] * 3 + [w_tail] * 3 + [jnp.zeros((LANES - 3 * TAIL, f_hid), BF16)])
        vmem = pl.BlockSpec(memory_space=pltpu.VMEM)
        partial = pl.pallas_call(
            backward_kernel,
            in_specs=[SMEM, whole, vmem, vmem, vmem, whole, whole],
            out_specs=vmem,
            out_shape=jax.ShapeDtypeStruct((f_in + pad, f_hid), F32),
            scratch_shapes=[
                pltpu.VMEM((n * 2, LANES), F32),
                pltpu.VMEM((n, f_hid), BF16),
                pltpu.VMEM((n, f_in), BF16),
                dma,
                dma((2, n // BLOCK)),
            ],
            compiler_params=pltpu.CompilerParams(vmem_limit_bytes=44 * 2**20),
            name="backward",
        )(lists2, ext_grad, back, w_parts, gw_two, h_one, z_one)
        total = reduce_all(partial)
        return -total[f_in + pad - 1, 0] / label_total, total[:f_in], total[f_in : f_in + classes].T

    row_spec = P("graph", None)
    vec_spec = P("graph")
    return jax.shard_map(
        device_step,
        mesh=mesh,
        in_specs=(row_spec, P(), P(), row_spec, vec_spec, row_spec, row_spec, vec_spec, vec_spec),
        out_specs=(P(), P(), P()),
        check_vma=False,
    )
```

```python
import functools

import jax
import jax.numpy as jnp
from jax import lax
from jax.experimental import pallas as pl
from jax.experimental.pallas import tpu as pltpu
from jax.sharding import PartitionSpec as P

LANES = 128
TAIL = 32
STEP = 16
BLOCK = 512
CHUNK = 512
F32, BF16 = jnp.float32, jnp.bfloat16


def once(shape):
    return pl.BlockSpec(shape, lambda g: (0,) * len(shape), pipeline_mode=pl.Buffered(1))


def fill_rows(dst, src, offset, blocks):
    def step(i, carry):
        r = pl.multiple_of(i * 64, 64)
        x = src[pl.ds(r, 64), :].astype(F32)
        for c in range(blocks):
            dst[pl.ds((r + offset) * 8 + c, 64, stride=8), :] = x[:, c * LANES : (c + 1) * LANES]
        return carry

    lax.fori_loop(0, src.shape[0] // 64, step, 0)


def put_weights(wbuf, w):
    deg = w.shape[1]
    for h in range(STEP // 8):
        for k in range(deg):
            tile = jnp.broadcast_to(w[h * 8 : h * 8 + 8, k : k + 1], (8, LANES))
            wbuf[pl.ds((h * deg + k) * 8, 8), :] = tile


def gather_rows(steps, row_of, src, wt, table, out, wbuf):
    deg = wt.shape[1]

    def put(i):
        put_weights(wbuf, wt[pl.ds(pl.multiple_of(i * STEP, STEP), STEP), :])

    put(0)

    def step(i, carry):
        dst = out.at[pl.ds(pl.multiple_of(i * STEP * 8, STEP * 8), STEP * 8)]
        for u in range(STEP):
            n = row_of(i * STEP + u)
            acc = None
            for k in range(deg):
                row = table[pl.ds(pl.multiple_of(src[k][n], 8), 8), :]
                term = row * wbuf[pl.ds((u // 8 * deg + k) * 8 + u % 8, 8, stride=0), :]
                acc = term if acc is None else acc + term
            dst[pl.ds(u * 8, 8), :] = acc
        put(jnp.minimum(i + 1, steps - 1))
        return carry

    lax.fori_loop(0, steps, step, 0)


def load_sources(src_hbm, src, sems):
    copies = [pltpu.make_async_copy(hbm, ref, sems.at[k]) for k, (hbm, ref) in enumerate(zip(src_hbm, src))]
    for copy in copies:
        copy.start()
    return copies


def fill_tiles(dst, src, offset):
    def step(i, carry):
        at = pl.multiple_of(i * 128, 128)
        dst[pl.ds(pl.multiple_of(offset * 8 + at, 8), 128), :] = src[pl.ds(at, 128), :].astype(F32)
        return carry

    lax.fori_loop(0, src.shape[0] // 128, step, 0)


def fill_from(table, hbm, chunk, sems, blocks):
    rows = chunk.shape[1]
    steps = hbm.shape[0] // rows

    def fetch(i):
        slot = lax.rem(i, 2)
        return pltpu.make_async_copy(hbm.at[pl.ds(pl.multiple_of(i * rows, rows), rows), :], chunk.at[slot], sems.at[slot])

    fetch(0).start()

    def take(i, carry):
        @pl.when(i + 1 < steps)
        def _():
            fetch(i + 1).start()

        fetch(i).wait()
        slot = lax.rem(i, 2)

        def fill(j, carry):
            r = pl.multiple_of(j * 64, 64)
            x = chunk[slot, pl.ds(r, 64), :].astype(F32)
            for c in range(blocks):
                table[pl.ds((i * rows + r) * 8 + c, 64, stride=8), :] = x[:, c * LANES : (c + 1) * LANES]
            return carry

        return lax.fori_loop(0, rows // 64, fill, carry)

    lax.fori_loop(0, steps, take, 0)


def first_layer(zbuf, w, rows, blocks):
    z = jnp.concatenate([zbuf[pl.ds(c, rows, stride=8), :] for c in range(blocks)], axis=1).astype(BF16)
    return z, jnp.maximum(jnp.dot(z, w[...], preferred_element_type=F32), 0.0)


def list_rows_kernel(deg, lists, *refs):
    src_hbm, refs, src = refs[:deg], refs[deg:-deg], refs[-deg:]
    feats, halo, wt, w, second, table, zbuf, wbuf, list_wt, chunk, src_sem, chunk_sem = refs
    rows, blocks = list_wt.shape[0], feats.shape[1] // LANES
    index_copies = load_sources(src_hbm, src, src_sem)
    fill_rows(table, halo, feats.shape[0], blocks)
    fill_from(table, feats, chunk, chunk_sem, blocks)

    def pick(i, carry):
        for u in range(8):
            j = i * 8 + u
            list_wt[pl.ds(j, 1), :] = wt[pl.ds(lists[j], 1), :]
        return carry

    lax.fori_loop(0, rows // 8, pick, 0)
    for copy in index_copies:
        copy.wait()
    gather_rows(rows // STEP, lambda j: lists[j], src, list_wt, table, zbuf, wbuf)
    _, h = first_layer(zbuf, w, rows, blocks)
    for c in range(h.shape[1] // LANES):
        zbuf[pl.ds(c, rows, stride=8), :] = h[:, c * LANES : (c + 1) * LANES]
    second[...] = zbuf[...].astype(BF16)


def layer_one_kernel(deg, *refs):
    src_hbm, refs, src = refs[:deg], refs[deg:-deg], refs[-deg:]
    feats, halo, wt, w, z_out, h_out, table, zbuf, wbuf, chunk, src_sem, chunk_sem = refs
    g = pl.program_id(0)
    rows, blocks = z_out.shape[0], feats.shape[1] // LANES

    @pl.when(g == 0)
    def _():
        index_copies = load_sources(src_hbm, src, src_sem)
        fill_rows(table, halo, feats.shape[0], blocks)
        fill_from(table, feats, chunk, chunk_sem, blocks)
        for copy in index_copies:
            copy.wait()

    first_row = pl.multiple_of(g * rows, rows)
    gather_rows(rows // STEP, lambda j: first_row + j, src, wt, table, zbuf, wbuf)
    z, h = first_layer(zbuf, w, rows, blocks)
    z_out[...] = z
    h_out[...] = h.astype(BF16)


def layer_two_kernel(classes, deg, label_total, *refs):
    src_hbm, refs, src = refs[:deg], refs[deg:-deg], refs[-deg:]
    wt, own, halo, w, label, g_out, z_out, loss_out, table, zbuf, wbuf, loss_sum, chunk, src_sem, chunk_sem = refs
    g = pl.program_id(0)
    rows, blocks = g_out.shape[0], own.shape[1] // LANES

    @pl.when(g == 0)
    def _():
        index_copies = load_sources(src_hbm, src, src_sem)
        loss_sum[...] = jnp.zeros_like(loss_sum)
        fill_tiles(table, halo, own.shape[0])
        fill_from(table, own, chunk, chunk_sem, blocks)
        for copy in index_copies:
            copy.wait()

    first_row = g * rows
    gather_rows(rows // STEP, lambda j: first_row + j, src, wt, table, zbuf, wbuf)
    z = jnp.concatenate([zbuf[pl.ds(c, rows, stride=8), :] for c in range(blocks)], axis=1).astype(BF16)
    logits = jnp.dot(z, w[...], preferred_element_type=F32)
    col = lax.broadcasted_iota(jnp.int32, logits.shape, 1)
    real = col < classes
    top = jnp.max(jnp.where(real, logits, -jnp.inf), axis=1, keepdims=True)
    shifted = logits - top
    log_sum = jnp.log(jnp.sum(jnp.where(real, jnp.exp(shifted), 0.0), axis=1, keepdims=True))
    log_prob = shifted - log_sum
    tag = label[...]
    hit = col == tag
    loss_sum[...] += jnp.sum(jnp.where(hit, log_prob, 0.0), axis=0, keepdims=True)
    scale = jnp.where(tag >= 0, (1.0 / label_total[...])[:, :1], 0.0)
    grad = jnp.where(real, (jnp.exp(log_prob) - jnp.where(hit, 1.0, 0.0)) * scale, 0.0).astype(BF16)
    g_out[...] = grad
    z_out[...] = z

    @pl.when(g == pl.num_programs(0) - 1)
    def _():
        loss_out[...] = jnp.broadcast_to(jnp.sum(loss_sum[...], axis=1, keepdims=True), loss_out.shape)


def grad_two_kernel(grad, z, loss, gw_out):
    g = pl.program_id(0)

    @pl.when(g == 0)
    def _():
        gw_out[...] = jnp.zeros_like(gw_out)

    gw_out[...] += lax.dot_general(grad[...], z[...], (((0,), (0,)), ((), ())), preferred_element_type=F32)

    @pl.when(g == pl.num_programs(0) - 1)
    def _():
        gw_out[pl.ds(gw_out.shape[0] - 1, 1), pl.ds(0, LANES)] = loss[...]


def scatter_kernel(deg, *refs):
    src_hbm, (wt, grad, own_out, back_out, gbuf, wbuf, sems), refs = refs[:deg], refs[deg : deg + 7], refs[deg + 7 :]
    src, parts = refs[:deg], refs[deg:]
    g = pl.program_id(0)
    rows = grad.shape[0]
    steps = rows // STEP

    @pl.when(g == 0)
    def _():
        index_copies = load_sources(src_hbm, src, sems)

        def clear(i, carry):
            for part in parts:
                for j in range(8):
                    part[pl.ds(pl.multiple_of(i * 64, 64) + j * 8, 8), :] = jnp.zeros((8, LANES), F32)
            return carry

        lax.fori_loop(0, parts[0].shape[0] // 64, clear, 0)
        for copy in index_copies:
            copy.wait()

    x = grad[...].astype(F32)
    for c in range(2):
        gbuf[pl.ds(c, rows, stride=2), :] = x[:, c * LANES : (c + 1) * LANES]

    def put(i):
        put_weights(wbuf, wt[pl.ds(pl.multiple_of(i * STEP, STEP), STEP), :])

    put(0)

    def step(i, carry):
        here = gbuf.at[pl.ds(pl.multiple_of(i * STEP * 2, STEP * 2), STEP * 2)]
        for u in range(STEP):
            row = here[pl.ds(u * 2, 2), :]
            n = g * rows + i * STEP + u
            for k in range(deg):
                at = pl.ds(pl.multiple_of(src[k][n], 2), 2)
                w = wbuf[pl.ds((u // 8 * deg + k) * 8 + u % 8, 2, stride=0), :]
                parts[k][at, :] = parts[k][at, :] + row * w
        put(jnp.minimum(i + 1, steps - 1))
        return carry

    lax.fori_loop(0, steps, step, 0)

    @pl.when(g == pl.num_programs(0) - 1)
    def _():
        def add_into(dst, offset):
            def add(i, carry):
                at = pl.multiple_of(i * 64, 64)
                rows_at = pl.ds(pl.multiple_of(at + offset, 64), 64)
                total = parts[0][rows_at, :]
                for part in parts[1:]:
                    total = total + part[rows_at, :]
                dst[pl.ds(at, 64), :] = total
                return carry

            lax.fori_loop(0, dst.shape[0] // 64, add, 0)

        add_into(own_out, 0)
        add_into(back_out, own_out.shape[0])


def backward_kernel(lists, own, back, w_t, gw_two, h_hbm, z_hbm, gw_out, total, h, z, own_sem, sems):
    n, f_in = z.shape
    rows = CHUNK
    own_copy = pltpu.make_async_copy(own, total, own_sem)
    own_copy.start()

    def fetch(i):
        at = pl.ds(pl.multiple_of(i * rows, rows), rows)
        return (
            pltpu.make_async_copy(h_hbm.at[at], h.at[at], sems.at[0, i]),
            pltpu.make_async_copy(z_hbm.at[at], z.at[at], sems.at[1, i]),
        )

    def begin(i, carry):
        for copy in fetch(i):
            copy.start()
        return carry

    lax.fori_loop(0, n // rows, begin, 0)
    gw_out[pl.ds(0, f_in), :] = jnp.zeros((f_in, gw_out.shape[1]), F32)
    gw_out[pl.ds(f_in, gw_two.shape[0]), :] = gw_two[...]

    own_copy.wait()

    def add(i, carry):
        for j in range(4):
            at = pl.ds(pl.multiple_of(lists[i * 4 + j], 2), 2)
            total[at, :] = total[at, :] + back[pl.ds(pl.multiple_of(i * 8, 8) + j * 2, 2), :]
        return carry

    lax.fori_loop(0, back.shape[0] // 8, add, 0)

    def block(i, carry):
        for copy in fetch(i):
            copy.wait()
        at = pl.ds(pl.multiple_of(i * rows, rows), rows)
        parts = []
        for c in range(2):
            s = total[pl.ds(i * rows * 2 + c, rows, stride=2), :]
            high = s.astype(BF16).astype(F32)
            mid = (s - high).astype(BF16).astype(F32)
            parts.append((high, mid, s - high - mid))
        tail = parts[1][0] + pltpu.roll(parts[1][1], TAIL, 1) + pltpu.roll(parts[1][2], 2 * TAIL, 1)
        d = jnp.dot(jnp.concatenate([*parts[0], tail], axis=1).astype(BF16), w_t[...], preferred_element_type=F32)
        grad = jnp.where(h[at, :] > 0, d, 0.0).astype(BF16)
        gw_out[pl.ds(0, f_in), :] += lax.dot_general(z[at, :], grad, (((0,), (0,)), ((), ())), preferred_element_type=F32)
        return carry

    lax.fori_loop(0, n // rows, block, 0)


MESH = pl.DeviceIdType.MESH
SIDE = 4
COLORS = (
    (0, 256, (0, 1, 2)),
    (256, 128, (1, 2, 0)),
    (384, 128, (2, 0, 1)),
    (512, 128, (0, 1, 2)),
    (640, 256, (1, 2, 0)),
    (896, 128, (2, 0, 1)),
)
SETS = ((0, 1, 2), (3, 4, 5))


def reduce_kernel(x, out, acc, pair_buf, relay, far, mid, near, *sems):
    pair_send, pair_recv, ring_send, ring_recv, rs_send, rs_recv, ag_send, ag_recv, back_send, back_recv = sems
    me = lax.axis_index("graph")
    core = lax.rem(me, 2)
    where = [lax.rem(me // (2 * SIDE**d), SIDE) for d in range(3)]
    partner = me + 1 - 2 * core
    half = acc.shape[0]
    big = half // SIDE

    def peer(axis, t):
        p = lax.rem(where[axis] + t, SIDE)
        return p, me + (p - where[axis]) * (2 * SIDE**axis)

    barrier = pltpu.get_barrier_semaphore()
    pl.semaphore_signal(barrier, inc=1, device_id=(partner,), device_id_type=MESH)
    for axis in range(3):
        for t in range(1, SIDE):
            pl.semaphore_signal(barrier, inc=1, device_id=(peer(axis, t)[1],), device_id_type=MESH)
    pl.semaphore_wait(barrier, 10)
    pending = []

    def send(src, dst, send_sem, recv_sem, dev):
        copy = pltpu.make_async_remote_copy(
            src_ref=src, dst_ref=dst, send_sem=send_sem, recv_sem=recv_sem, device_id=(dev,), device_id_type=MESH
        )
        copy.start()
        pending.append(copy)
        return copy

    base, other = pl.multiple_of(core * half, 8), pl.multiple_of(half - core * half, 8)
    colors = [(pl.ds(lane, width), axes) for lane, width, axes in COLORS]

    def piece(c, t, part, start=0):
        p, _ = peer(colors[c][1][0], t)
        return pl.ds(pl.multiple_of(start + p * big + part * (big // 2), 8), big // 2)

    order = ((2, 0), (2, 1), (1, 1), (3, 0), (1, 0), (3, 1), (0, 0), (0, 1))
    pair, ring, later, got = {}, {}, {}, {}
    for phase in (order[:4], order[4:]):
        for group in SETS:
            for t, part in phase:
                for c in group:
                    lanes = colors[c][0]
                    at = piece(c, t, part)
                    slot = (c, t * 2 + part)
                    src = x.at[piece(c, t, part, other), lanes]
                    pair[c, t, part] = send(src, pair_buf.at[at, lanes], pair_send.at[slot], pair_recv.at[slot], partner)

    def first_axis(c, t, part):
        lanes, axes = colors[c]
        at = piece(c, t, part)
        pair[c, t, part].wait_recv()
        mine = x[piece(c, t, part, base), lanes] + pair_buf[at, lanes]
        if (t, part) in ((1, 0), (3, 1)):
            ring[c, 2, part].wait_recv()
            mine = mine + relay[part, :, lanes]
        acc[at, lanes] = mine
        if t == 0:
            return
        forward = part == 0 if t == 2 else t == 1
        _, dev = peer(axes[0], 1 if forward else 3)
        if t == 2:
            dst = relay.at[part, :, lanes]
        else:
            dst = far.at[0 if forward else 1, pl.ds(part * (big // 2), big // 2), lanes]
        slot = order.index((t, part))
        ring[c, t, part] = send(acc.at[at, lanes], dst, ring_send.at[0, c, slot], ring_recv.at[0, c, slot], dev)

    for phase in (order[:4], order[4:]):
        for group in SETS:
            for t, part in phase:
                for c in group:
                    first_axis(c, t, part)
    start = [where[axes[0]] * big for _, axes in colors]
    sizes = (big, big // SIDE, big // SIDE**2)
    bufs = (far, mid, near)

    def collect(stage, c):
        lanes, axes = colors[c]
        if stage:
            start[c] = start[c] + where[axes[stage]] * sizes[stage]
            for t in (1, 2, 3):
                later[c, t].wait_recv()
        else:
            for key in ((1, 1), (3, 0), (1, 0), (3, 1)):
                ring[(c, *key)].wait_recv()
        rows = pl.ds(pl.multiple_of(start[c], 8), sizes[stage])
        mine = acc[rows, lanes]
        for j in range(bufs[stage].shape[0]):
            mine = mine + bufs[stage][j, :, lanes]
        if stage < 2:
            acc[rows, lanes] = mine
        else:
            out[pl.ds(pl.multiple_of(base + start[c], 8), sizes[2]), lanes] = mine

    def scatter_on(stage, c):
        lanes, axes = colors[c]
        for t in (2, 1, 3):
            p, dev = peer(axes[stage], t)
            rows = pl.ds(pl.multiple_of(start[c] + p * sizes[stage], 8), sizes[stage])
            slot = (stage - 1, c, t - 1)
            later[c, t] = send(acc.at[rows, lanes], bufs[stage].at[t - 1, :, lanes], rs_send.at[slot], rs_recv.at[slot], dev)

    def spread(stage, c):
        lanes, axes = colors[c]
        here = out.at[pl.ds(pl.multiple_of(base + start[c], 8), sizes[stage]), lanes]
        for t in (2, 1, 3):
            _, dev = peer(axes[stage], t)
            slot = (stage - 1, c, t - 1)
            later[c, t] = send(here, here, ag_send.at[slot], ag_recv.at[slot], dev)

    def spread_done(stage, c):
        for t in (1, 2, 3):
            later[c, t].wait_recv()
        start[c] = start[c] - where[colors[c][1][stage]] * sizes[stage]

    def pass_on(c, t, part, slot, directions):
        here = out.at[piece(c, t, part, base), colors[c][0]]
        for d, name in directions:
            _, dev = peer(colors[c][1][0], d)
            got[c, name] = send(here, here, ring_send.at[1, c, name], ring_recv.at[1, c, name], dev)
        got[c, slot] = send(here, here, back_send.at[c, slot - 6], back_recv.at[c, slot - 6], partner)

    for group in SETS:
        for c in group:
            collect(0, c)
            scatter_on(1, c)
    for group in SETS:
        for c in group:
            collect(1, c)
            scatter_on(2, c)
    for group in SETS:
        for c in group:
            collect(2, c)
            spread(2, c)
    for group in SETS:
        for c in group:
            spread_done(2, c)
            spread(1, c)
    for group in SETS:
        for c in group:
            spread_done(1, c)
            pass_on(c, 0, 0, 6, ((1, 0), (3, 3)))
            pass_on(c, 0, 1, 7, ((3, 2), (1, 1)))
    for group in SETS:
        for c in group:
            got[c, 0].wait_recv()
            pass_on(c, 3, 0, 8, ((1, 4),))
            got[c, 2].wait_recv()
            pass_on(c, 1, 1, 9, ((3, 5),))
    for group in SETS:
        for name, (t, part), slot in ((1, (3, 1), 10), (3, (1, 0), 11), (4, (2, 0), 12), (5, (2, 1), 13)):
            for c in group:
                got[c, name].wait_recv()
                pass_on(c, t, part, slot, ())
    for c in range(len(colors)):
        for slot in range(6, 14):
            got[c, slot].wait_recv()
    for copy in pending:
        copy.wait_send()


def reduce_all(x):
    sem = pltpu.SemaphoreType.DMA
    return pl.pallas_call(reduce_kernel,
        in_specs=[pl.BlockSpec(memory_space=pltpu.VMEM)], out_specs=pl.BlockSpec(memory_space=pltpu.VMEM),
        out_shape=jax.ShapeDtypeStruct((1024,1024),F32),
        scratch_shapes=[pltpu.VMEM((512,1024),F32), pltpu.VMEM((512,1024),F32), pltpu.VMEM((2,64,1024),F32), pltpu.VMEM((2,128,1024),F32), pltpu.VMEM((3,32,1024),F32), pltpu.VMEM((3,8,1024),F32),
            sem((6,8)), sem((6,8)), sem((2,6,6)), sem((2,6,6)), sem((2,6,3)), sem((2,6,3)), sem((2,6,3)), sem((2,6,3)), sem((6,8)), sem((6,8))],
        compiler_params=pltpu.CompilerParams(collective_id=0, has_side_effects=True, vmem_limit_bytes=12*2**20),
        name="reduce_all")(x)


def exchange_kernel(n_dev, rows, count, w_hbm, wt_t, labels, mask, rows_in, total, w_out, wt_out, tag_out, came, w_f32, w, wt, tag, sems, local):
    me = lax.axis_index("graph")
    pairs = ((rows, rows_in), (count, came))
    load = pltpu.make_async_copy(w_hbm, w_f32, local.at[0])
    load.start()

    def send(t, carry):
        q = lax.rem(me + t, n_dev)
        for j, (src, dst) in enumerate(pairs):
            pltpu.make_async_remote_copy(
                src_ref=src.at[q if j == 0 else 0],
                dst_ref=dst.at[me],
                send_sem=sems.at[2 * j],
                recv_sem=sems.at[2 * j + 1],
                device_id=(q,),
                device_id_type=MESH,
            ).start()
        return carry

    lax.fori_loop(1, n_dev, send, 0)
    load.wait()
    w[...] = w_f32[...].astype(BF16)
    stores = [pltpu.make_async_copy(src, dst, local.at[j]) for j, (src, dst) in enumerate(((w, w_out), (wt, wt_out), (tag, tag_out)), 1)]
    stores[0].start()

    def turn(i, carry):
        at = pl.ds(pl.multiple_of(i * LANES, LANES), LANES)
        wt[at, :] = wt_t[:, at].T
        return carry

    lax.fori_loop(0, wt.shape[0] // LANES, turn, 0)
    stores[1].start()
    tags = jnp.where(mask[...] == 1, labels[...], -1).astype(F32).T.astype(jnp.int32)
    for j in range(tags.shape[1]):
        tag[pl.ds(j * LANES, LANES), :] = tags[:, j : j + 1]
    stores[2].start()
    came[me] = count[0]
    for j, (_, dst) in enumerate(pairs):
        others = dst.at[pl.ds(0, n_dev - 1)]
        for side in range(2):
            pltpu.make_async_copy(others, others, sems.at[2 * j + side]).wait()
    total[...] = jnp.sum(came[...], axis=0)
    for copy in stores:
        copy.wait()


def exchange(rows, count, w, wt_t, labels, mask):
    n_dev, (deg, n) = rows.shape[0], wt_t.shape
    vmem, hbm = pl.BlockSpec(memory_space=pltpu.VMEM), pl.BlockSpec(memory_space=pltpu.HBM)
    return pl.pallas_call(
        functools.partial(exchange_kernel, n_dev),
        in_specs=[vmem, vmem, hbm, vmem, vmem, vmem],
        out_specs=[vmem, vmem, hbm, hbm, hbm],
        out_shape=[
            jax.ShapeDtypeStruct(rows.shape, rows.dtype),
            jax.ShapeDtypeStruct((1, LANES), F32),
            jax.ShapeDtypeStruct(w.shape, BF16),
            jax.ShapeDtypeStruct((n, deg), F32),
            jax.ShapeDtypeStruct((n, 1), jnp.int32),
        ],
        scratch_shapes=[
            pltpu.VMEM((n_dev, 1, LANES), F32),
            pltpu.VMEM(w.shape, F32),
            pltpu.VMEM(w.shape, BF16),
            pltpu.VMEM((n, deg), F32),
            pltpu.VMEM((n, 1), jnp.int32),
            pltpu.SemaphoreType.DMA((4,)),
            pltpu.SemaphoreType.DMA((4,)),
        ],
        compiler_params=pltpu.CompilerParams(has_side_effects=True, vmem_limit_bytes=62 * 2**20),
        name="exchange_one",
    )(rows, count, w, wt_t, labels.reshape(-1, LANES), mask.reshape(-1, LANES))


def params():
    return pltpu.CompilerParams(dimension_semantics=("arbitrary",), vmem_limit_bytes=62 * 2**20)


SMEM = pl.BlockSpec(memory_space=pltpu.SMEM)


def solution(mesh):
    dev_count = mesh.shape["graph"]

    def device_step(feats, w_one, w_two, send_idx, send_count, edge_src, edge_wt, labels, label_mask):
        n, f_in = feats.shape
        f_hid, classes = w_two.shape
        halo_rows, deg = send_idx.shape[1], edge_src.shape[1]
        halo = dev_count * halo_rows
        ext = n + halo
        pad = 2 * LANES
        w_two_b = jnp.pad(w_two.astype(BF16), ((0, 0), (0, pad - classes)))
        list_ids = send_idx.reshape(halo)
        lists2 = list_ids * 2
        src8 = [edge_src[:, k] * 8 for k in range(deg)]
        src2 = [edge_src[:, k] * 2 for k in range(deg)]
        count = jnp.sum(label_mask.astype(F32))
        first_rows = feats[list_ids].reshape(dev_count, halo_rows, f_in)
        first_in, label_total, w_one_b, wt, label = exchange(
            first_rows, jnp.full((1, 1, LANES), count), w_one, edge_wt.T, labels, label_mask
        )
        first_in = first_in.reshape(halo, f_in)

        def by_rows(width):
            return pl.BlockSpec((BLOCK, width), lambda g: (g, 0))

        def gather_scratch(rows):
            return [pltpu.VMEM((ext * 8, LANES), F32), pltpu.VMEM((rows * 8, LANES), F32), pltpu.VMEM((STEP * deg + 8, LANES), F32)]

        whole = pl.BlockSpec(memory_space=pl.ANY)
        dma = pltpu.SemaphoreType.DMA
        index_scratch = [pltpu.SMEM((n,), jnp.int32) for _ in range(deg)]

        def chunk_scratch(width):
            return [pltpu.VMEM((2, CHUNK, width), BF16), dma((deg,)), dma((2,))]

        second = pl.pallas_call(
            functools.partial(list_rows_kernel, deg),
            grid=(1,),
            in_specs=[SMEM] + [whole] * (deg + 1) + [once((halo, f_in)), once((n, deg)), once((f_in, f_hid))],
            out_specs=once((halo * 8, LANES)),
            out_shape=jax.ShapeDtypeStruct((halo * 8, LANES), BF16),
            scratch_shapes=gather_scratch(halo) + [pltpu.VMEM((halo, deg), F32)] + chunk_scratch(f_in) + index_scratch,
            compiler_params=params(),
            cost_estimate=pl.CostEstimate(flops=4 * halo * f_in * f_hid, bytes_accessed=2 * n * f_in, transcendentals=0),
            name="list_rows",
        )(list_ids, *src8, feats, first_in, wt, w_one_b)
        h_in = lax.all_to_all(second, "graph", 0, 0, tiled=True)
        z_one, h_one = pl.pallas_call(
            functools.partial(layer_one_kernel, deg),
            grid=(n // BLOCK,),
            in_specs=[whole] * (deg + 1) + [once((halo, f_in)), by_rows(deg), once((f_in, f_hid))],
            out_specs=[by_rows(f_in), by_rows(f_hid)],
            out_shape=[jax.ShapeDtypeStruct((n, f_in), BF16), jax.ShapeDtypeStruct((n, f_hid), BF16)],
            scratch_shapes=gather_scratch(BLOCK) + chunk_scratch(f_in) + index_scratch,
            compiler_params=params(),
            cost_estimate=pl.CostEstimate(flops=8 * n * f_in * f_hid, bytes_accessed=8 * n * f_in, transcendentals=0),
            name="layer_one",
        )(*src8, feats, first_in, wt, w_one_b)
        grad_log, z_two, loss_part = pl.pallas_call(
            functools.partial(layer_two_kernel, classes, deg),
            grid=(n // BLOCK,),
            in_specs=[once((1, LANES))] + [whole] * deg + [by_rows(deg), whole, once((halo * 8, LANES)), once((f_hid, pad)), by_rows(1)],
            out_specs=[by_rows(pad), by_rows(f_hid), once((1, LANES))],
            out_shape=[
                jax.ShapeDtypeStruct((n, pad), BF16),
                jax.ShapeDtypeStruct((n, f_hid), BF16),
                jax.ShapeDtypeStruct((1, LANES), F32),
            ],
            scratch_shapes=gather_scratch(BLOCK) + [pltpu.VMEM((1, pad), F32)] + chunk_scratch(f_hid) + index_scratch,
            compiler_params=params(),
            name="layer_two",
        )(label_total, *src8, wt, h_one, h_in, w_two_b, label)
        own_grad, returned = pl.pallas_call(
            functools.partial(scatter_kernel, deg),
            grid=(n // 512,),
            in_specs=[whole] * deg + [by_rows(deg), by_rows(pad)],
            out_specs=[once((n * 2, LANES)), once((halo * 2, LANES))],
            out_shape=[jax.ShapeDtypeStruct((n * 2, LANES), F32), jax.ShapeDtypeStruct((halo * 2, LANES), F32)],
            scratch_shapes=[pltpu.VMEM((BLOCK * 2, LANES), F32), pltpu.VMEM((STEP * deg + 8, LANES), F32), dma((deg,))]
            + index_scratch
            + [pltpu.VMEM((ext * 2, LANES), F32) for _ in range(deg)],
            compiler_params=params(),
            name="scatter",
        )(*src2, wt, grad_log)
        returned, grad_log = lax.optimization_barrier((returned, grad_log))
        back = lax.all_to_all(returned, "graph", 0, 0, tiled=True)
        gw_two = pl.pallas_call(
            grad_two_kernel,
            grid=(n // BLOCK,),
            in_specs=[by_rows(pad), by_rows(f_hid), once((1, LANES))],
            out_specs=once((pad, f_hid)),
            out_shape=jax.ShapeDtypeStruct((pad, f_hid), F32),
            compiler_params=pltpu.CompilerParams(dimension_semantics=("arbitrary",), vmem_limit_bytes=20 * 2**20),
            cost_estimate=pl.CostEstimate(flops=2 * n * pad * f_hid, bytes_accessed=2 * n * f_hid, transcendentals=0),
            name="grad_two",
        )(grad_log, z_two, loss_part)
        w_t = w_two.astype(BF16).T
        w_tail = jnp.pad(w_t[LANES:], ((0, TAIL - (classes - LANES)), (0, 0)))
        w_parts = jnp.concatenate([w_t[:LANES]] * 3 + [w_tail] * 3 + [jnp.zeros((LANES - 3 * TAIL, f_hid), BF16)])
        vmem = pl.BlockSpec(memory_space=pltpu.VMEM)
        partial = pl.pallas_call(
            backward_kernel,
            in_specs=[SMEM, whole, vmem, vmem, vmem, whole, whole],
            out_specs=vmem,
            out_shape=jax.ShapeDtypeStruct((f_in + pad, f_hid), F32),
            scratch_shapes=[
                pltpu.VMEM((n * 2, LANES), F32),
                pltpu.VMEM((n, f_hid), BF16),
                pltpu.VMEM((n, f_in), BF16),
                dma,
                dma((2, n // CHUNK)),
            ],
            compiler_params=pltpu.CompilerParams(vmem_limit_bytes=44 * 2**20),
            name="backward",
        )(lists2, own_grad, back, w_parts, gw_two, h_one, z_one)
        total = reduce_all(partial)
        return -total[f_in + pad - 1, 0] / label_total[0, 0], total[:f_in], total[f_in : f_in + classes].T

    row_spec = P("graph", None)
    vec_spec = P("graph")
    return jax.shard_map(
        device_step,
        mesh=mesh,
        in_specs=(row_spec, P(), P(), row_spec, vec_spec, row_spec, row_spec, vec_spec, vec_spec),
        out_specs=(P(), P(), P()),
        check_vma=False,
    )
```
